32 devices in a mesh: dp: 8 (over y, x, core), mp: 4 (over z).
Axes of the slice: x: 2, y: 2, z: 4, core: 2. Of those that a mesh axis runs over, the one named last changes fastest.
Arguments:
- tokens: bfloat16 [2048, 6144], P('dp', 'mp'), may hold values from -40 to 40
- norm_gain: float32 [6144], P('mp'), may hold values from 0.1 to 1.9
- w_qkv: bfloat16 [6144, 3, 4096], P('mp', None, 'dp'), may hold values from -0.078125 to 0.078125
- w_up: bfloat16 [6144, 12288], P('mp', 'dp'), may hold values from -0.078125 to 0.078125
- w_attn_out: bfloat16 [4096, 6144], P('dp', 'mp'), may hold values from -0.09375 to 0.09375
- w_down: bfloat16 [12288, 6144], P('dp', 'mp'), may hold values from -0.0546875 to 0.0546875
Outputs:
- layer_out: bfloat16 [2048, 6144], P('dp', 'mp')
The draws below stay inside these ranges and needn't reach their ends.
All inputs are finite; a program needn't handle non-finite values.
Results may differ from the reference program's by a relative error of at most 0.015.
Values may be sent and summed in bfloat16 or wider, within the bound.
A program may use at most 128 MiB of HBM per device.

```python
import jax
import jax.numpy as jnp
from jax import lax

D = 6144
HEADS = 32
HEAD_DIM = 128
FF = 12288
PATCHES = 256
TOKENS = 2048
N_DP = 8
N_MP = 4


def draw_tokens(key, part):
    first = jax.random.fold_in(key, 0)
    ramp = 0.6 * 3.0 ** (jnp.arange(D, dtype=jnp.float32) / D)
    values = jnp.clip(jax.random.normal(first, (TOKENS, D), jnp.float32), -6.0, 6.0) * ramp[None, :]
    return values.astype(jnp.bfloat16)


def levels(own_key, extent, pieces, low, largest):
    level = 1.0
    for dim, blocks in pieces:
        steps = jax.random.uniform(jax.random.fold_in(jax.random.fold_in(own_key, 6), dim), (blocks,), jnp.float32, low / len(pieces), largest / len(pieces))
        level = level * jnp.repeat(jnp.exp(steps), extent[dim] // blocks).reshape((-1,) + (1,) * (len(extent) - 1 - dim))
    return level


def bell_draw(rng, dims, deviation, most, pieces=(), held_as=jnp.bfloat16):
    loudness = levels(rng, dims, pieces, -0.22, 0.18) if pieces else 1.0
    drawn = jax.random.normal(rng, dims, jnp.float32) * deviation * loudness
    return jnp.minimum(jnp.maximum(drawn, -most), most).astype(held_as)


def setup_inputs(seed: int = 0) -> dict:
    splits = jax.random.split(jax.random.key(seed), 7)
    return {
        "tokens": draw_tokens(jax.random.fold_in(splits[6], 71), 0),
        "norm_gain": jnp.clip(1.0 + 0.18 * jax.random.normal(splits[1], (D,), jnp.float32), 0.1, 1.9),
        "w_qkv": bell_draw(splits[2], (D, 3, HEADS * HEAD_DIM), D ** -0.5, 0.078125, ((0, 4), (2, 8))),
        "w_up": bell_draw(splits[3], (D, FF), D ** -0.5, 0.078125, ((0, 4), (1, 8))),
        "w_attn_out": bell_draw(splits[4], (HEADS * HEAD_DIM, D), (HEADS * HEAD_DIM) ** -0.5, 0.09375, ((0, 8), (1, 4))),
        "w_down": bell_draw(splits[5], (FF, D), FF ** -0.5, 0.0546875, ((0, 8), (1, 4))),
    }


EPS = 1e-06

def normalize_rows(values, total, squares, gain, width):
    mean = total / width
    spread = squares / width - mean * mean
    scaled = (values - mean[:, None]) * lax.rsqrt(spread + EPS)[:, None]
    return (scaled * gain[None, :]).astype(jnp.bfloat16)

def head_norm(values):
    mean = lax.optimization_barrier(jnp.mean(values, axis=-1, keepdims=True))
    centered = values - mean
    spread = lax.optimization_barrier(jnp.mean(centered * centered, axis=-1, keepdims=True))
    return centered * lax.rsqrt(spread + EPS)

def attend(qkv, heads_here):
    rows = qkv.shape[0]
    images = rows // PATCHES
    parts = qkv.reshape(images, PATCHES, 3, heads_here, HEAD_DIM)
    query = (head_norm(parts[:, :, 0].astype(jnp.float32)) * (1.0 / HEAD_DIM) ** 0.5).astype(jnp.bfloat16)
    keys = head_norm(parts[:, :, 1].astype(jnp.float32)).astype(jnp.bfloat16)
    values = parts[:, :, 2]
    scores = jnp.einsum('iqhd,ikhd->ihqk', query.astype(jnp.float32), keys.astype(jnp.float32))
    weights = jnp.exp(scores)
    probs = (weights / lax.optimization_barrier(jnp.sum(weights, axis=-1, keepdims=True))).astype(jnp.bfloat16)
    mixed = jnp.einsum('ihqk,ikhd->iqhd', probs.astype(jnp.float32), values.astype(jnp.float32))
    return mixed.astype(jnp.bfloat16).reshape(rows, heads_here * HEAD_DIM)

def reference(tokens, norm_gain, w_qkv, w_up, w_attn_out, w_down):
    xf = tokens.astype(jnp.float32)
    normed = normalize_rows(xf, lax.optimization_barrier(jnp.sum(xf, axis=1)), lax.optimization_barrier(jnp.sum(xf * xf, axis=1)), norm_gain, D)
    head_cols = HEADS * HEAD_DIM
    w_heads = w_qkv.reshape(D, 3 * head_cols)
    feat_block = D // N_MP
    projected = jnp.zeros((TOKENS, 3 * head_cols + FF), jnp.float32)
    for block in range(N_MP):
        first = block * feat_block
        cols = normed[:, first:first + feat_block]
        term = jnp.concatenate([jnp.dot(cols, w_heads[first:first + feat_block], preferred_element_type=jnp.float32), jnp.dot(cols, w_up[first:first + feat_block], preferred_element_type=jnp.float32)], axis=1)
        projected = projected + lax.optimization_barrier(term.astype(jnp.bfloat16)).astype(jnp.float32)
    projected = projected.astype(jnp.bfloat16)
    qkv = projected[:, :3 * head_cols].reshape(TOKENS, 3, head_cols)
    attended = attend(qkv, HEADS)
    activated = jax.nn.gelu(projected[:, 3 * head_cols:].astype(jnp.float32)).astype(jnp.bfloat16)
    head_block = head_cols // N_DP
    unit_block = FF // N_DP
    total = xf
    for block in range(N_DP):
        hfirst = block * head_block
        ufirst = block * unit_block
        term = jnp.dot(attended[:, hfirst:hfirst + head_block], w_attn_out[hfirst:hfirst + head_block], preferred_element_type=jnp.float32)
        term = term + jnp.dot(activated[:, ufirst:ufirst + unit_block], w_down[ufirst:ufirst + unit_block], preferred_element_type=jnp.float32)
        total = total + lax.optimization_barrier(term.astype(jnp.bfloat16)).astype(jnp.float32)
    return total.astype(jnp.bfloat16)
```

```python
import functools

import jax
import jax.numpy as jnp
from jax import lax
from jax.experimental import pallas as pl
from jax.experimental.pallas import tpu as pltpu
from jax.sharding import PartitionSpec as P

MESH = pl.DeviceIdType.MESH

HEAD_DIM = 128
PATCHES = 256


EPS = 1e-06
UP_SHARES = (1, 2, 2, 1)
FIRST = 1
LAG = 2


def normalize_rows(values, total, squares, gain, width):
    mean = total / width
    spread = squares / width - mean * mean
    scaled = (values - mean[:, None]) * lax.rsqrt(spread + EPS)[:, None]
    return (scaled * gain[None, :]).astype(jnp.bfloat16)


def head_norm(values):
    mean = jnp.mean(values, axis=-1, keepdims=True)
    centered = values - mean
    spread = jnp.mean(centered * centered, axis=-1, keepdims=True)
    return centered * lax.rsqrt(spread + EPS)


def attend(qkv, heads_here):
    rows = qkv.shape[0]
    images = rows // PATCHES
    parts = qkv.reshape(images, PATCHES, 3, heads_here, HEAD_DIM)
    query = (head_norm(parts[:, :, 0].astype(jnp.float32)) * (1.0 / HEAD_DIM) ** 0.5).astype(
        jnp.bfloat16
    )
    keys = head_norm(parts[:, :, 1].astype(jnp.float32)).astype(jnp.bfloat16)
    values = parts[:, :, 2]
    scores = jnp.einsum("iqhd,ikhd->ihqk", query, keys, preferred_element_type=jnp.float32)
    weights = jnp.exp(scores)
    probs = (weights / jnp.sum(weights, axis=-1, keepdims=True)).astype(jnp.bfloat16)
    mixed = jnp.einsum("ihqk,ikhd->iqhd", probs, values, preferred_element_type=jnp.float32)
    return mixed.astype(jnp.bfloat16).reshape(rows, heads_here * HEAD_DIM)


def shift(values, axis, senders, step):
    return lax.ppermute(values, axis, [(i, i + step) for i in senders])


def rows_of(values, block, count):
    return lax.dynamic_slice_in_dim(values, block * count, count, 0)


def add_rounded(*terms):
    total = terms[0].astype(jnp.float32)
    for term in terms[1:]:
        total = total + term.astype(jnp.float32)
    return total.astype(jnp.bfloat16)


class Group:
    def __init__(self, terms, finish, n, me, count):
        self.terms, self.finish, self.n, self.me, self.count = terms, finish, n, me, count
        self.right = self.left = self.own = None
        self.from_left, self.from_right = [], []

    def inputs(self, kind, step):
        n, me, count = self.n, self.me, self.count
        if kind == "scatter":
            send_right = rows_of(self.terms, (me - step - 1) % n, count)
            send_left = rows_of(self.terms, (me + step + 1) % n, count)
            if step:
                send_right = add_rounded(self.right, send_right)
                send_left = add_rounded(self.left, send_left)
            return send_right, send_left
        if step == 0:
            total = add_rounded(rows_of(self.terms, me, count), self.right, self.left)
            self.own = self.finish(total)
            return self.own, self.own
        return self.from_left[-1], self.from_right[-1]

    def move(self, kind, step, send_right, send_left):
        n = self.n
        if kind == "scatter":
            self.right = shift(send_right, "mp", range(step + 1), 1)
            self.left = shift(send_left, "mp", range(n - 1 - step, n), -1)
            return [self.right, self.left]
        self.from_left.append(shift(send_right, "mp", range(step, n - 1), 1))
        self.from_right.append(shift(send_left, "mp", range(1, n - step), -1))
        return [self.from_left[-1], self.from_right[-1]]

    def block(self, r):
        if r == 0:
            return self.own
        near, far = self.from_right[r - 1], self.from_left[self.n - r - 1]
        return jnp.where(self.me + r < self.n, near, far)


def run_line(groups, n):
    if n == 4:
        scatter_at, gather_at, period = [-3, -1, 0], [2, 5, 7], 4
    else:
        scatter_at, gather_at, period = [s - n + 2 for s in range(n - 1)], [2 + s for s in range(n - 1)], n
    slots = {}
    for g, group in enumerate(groups):
        for s in range(n - 1):
            slots.setdefault(g * period + gather_at[s], []).append((group, "gather", s))
            slots.setdefault(g * period + scatter_at[s], []).append((group, "scatter", s))
    history = []
    for at in sorted(slots):
        sends = [pair for group, kind, s in slots[at] for pair in group.inputs(kind, s)]
        if len(history) >= LAG:
            tied = lax.optimization_barrier(tuple(sends) + tuple(history[-LAG]))
            sends = tied[: len(sends)]
        moved = []
        for k, (group, kind, s) in enumerate(slots[at]):
            moved += group.move(kind, s, sends[2 * k], sends[2 * k + 1])
        history.append(moved)


def gather_normed(tokens, stats, n_dp, my_dp, normalize):
    rows, cols = tokens.shape
    if n_dp != 8:
        stats = lax.all_gather(stats, "dp", axis=1, tiled=True)
        return normalize(stats, lax.all_gather(tokens, "dp", axis=0, tiled=True), 0, n_dp)

    def hop(values, offset):
        return lax.ppermute(values, "dp", [(i, i ^ offset) for i in range(n_dp)])

    half = rows // 2
    held = {0: tokens, 2: hop(tokens, 2), 4: hop(tokens, 4)}
    held[1] = hop(tokens, 1)
    stats, held[2], held[4] = lax.optimization_barrier((stats, held[2], held[4]))
    stats = lax.all_gather(stats, "dp", axis=1, tiled=True)
    upper, lower = hop(held[2][:half], 4), hop(held[4][half:], 2)
    held[6] = jnp.concatenate([upper, lower])
    for offset in (2, 4, 6):
        held[offset ^ 1] = hop(held[offset], 1)
    result = jnp.zeros((n_dp * rows, cols), jnp.bfloat16)
    for offset in (0, 1, 2, 3, 4, 5, 6, 7):
        index = my_dp ^ offset
        result = lax.dynamic_update_slice_in_dim(
            result, normalize(stats, held[offset], index, 1), index * rows, 0
        )
    return result


def swap(values, bit, mine, dim, size):
    keep = lax.dynamic_index_in_dim(values, mine, dim, keepdims=False)
    give = lax.dynamic_index_in_dim(values, 1 - mine, dim, keepdims=False)
    got = lax.ppermute(give, "dp", [(i, i ^ (1 << bit)) for i in range(size)])
    return keep, got


def local(tokens, norm_gain, w_qkv, w_up, w_attn_out, w_down):
    if fits_line(tokens, w_qkv, w_up):
        return on_line(tokens, norm_gain, w_qkv, w_up, w_attn_out, w_down)
    n_mp, n_dp = lax.axis_size("mp"), lax.axis_size("dp")
    me, my_dp = lax.axis_index("mp"), lax.axis_index("dp")
    rows_here, feat_here = tokens.shape
    head_cols = w_qkv.shape[2]
    heads_here = head_cols // HEAD_DIM
    units = w_up.shape[1]
    width = feat_here * n_mp
    count = rows_here * n_dp // n_mp
    tokens_f = tokens.astype(jnp.float32)

    stats = lax.psum(
        jnp.stack([jnp.sum(tokens_f, axis=1), jnp.sum(tokens_f * tokens_f, axis=1)]), "mp"
    )

    def normalize(stats, block, index, many):
        here = lax.dynamic_slice_in_dim(stats, index * rows_here, many * rows_here, 1)
        return normalize_rows(block.astype(jnp.float32), here[0], here[1], norm_gain, width)

    normed = gather_normed(tokens, stats, n_dp, my_dp, normalize)

    halves = 2 if heads_here % 2 == 0 else 1
    group_heads = heads_here // halves
    group_cols = group_heads * HEAD_DIM

    def attention(projected):
        return attend(projected.reshape(count, 3, group_cols), group_heads)

    def activation(projected):
        return jax.nn.gelu(projected.astype(jnp.float32)).astype(jnp.bfloat16)

    heads = [("heads", g * group_cols, group_cols) for g in range(halves)]
    ups, first = [], 0
    for share in UP_SHARES:
        ups.append(("up", first, units * share // sum(UP_SHARES)))
        first += units * share // sum(UP_SHARES)
    groups = []
    weights_out = []
    for kind, start, size in ups[:FIRST] + heads + ups[FIRST:]:
        if kind == "heads":
            weight = w_qkv[:, :, start : start + size].reshape(feat_here, 3 * size)
            finish, weight_out = attention, w_attn_out[start : start + size]
        else:
            weight = w_up[:, start : start + size]
            finish, weight_out = activation, w_down[start : start + size]
        terms = jnp.dot(normed, weight, preferred_element_type=jnp.float32).astype(jnp.bfloat16)
        groups.append(Group(terms, finish, n_mp, me, count))
        weights_out.append(weight_out)
    run_line(groups, n_mp)

    order = sorted(range(n_mp), key=lambda r: min(r, n_mp - r))
    out_cols = w_down.shape[1]
    bits = n_dp.bit_length() - 1
    core = my_dp % 2
    pairs = count // rows_here // 2
    kept = jnp.zeros((n_mp * pairs, rows_here, out_cols), jnp.bfloat16)
    for r in order:
        block = sum(
            jnp.dot(group.block(r), weight, preferred_element_type=jnp.float32)
            for group, weight in zip(groups, weights_out)
        ).astype(jnp.bfloat16)
        block = block.reshape(pairs, 2, rows_here, out_cols)
        keep, got = swap(block, 0, core, 1, n_dp)
        kept = lax.dynamic_update_slice_in_dim(
            kept, add_rounded(keep, got), (me + r) % n_mp * pairs, 0
        )
    rest = list(range(1, bits))
    half = out_cols // 2
    results = []
    for part, bit_order in enumerate((rest, rest[::-1])):
        values = kept[:, :, part * half : (part + 1) * half].reshape(
            [2] * len(rest) + [rows_here, half]
        )
        left_bits = list(rest)
        base = tokens_f[:, part * half : (part + 1) * half]
        for bit in bit_order:
            dim = len(left_bits) - 1 - left_bits.index(bit)
            keep, got = swap(values, bit, (my_dp >> bit) % 2, dim, n_dp)
            left_bits.remove(bit)
            if left_bits:
                values = add_rounded(keep, got)
            else:
                total = base + (keep.astype(jnp.float32) + got.astype(jnp.float32))
                results.append(total.astype(jnp.bfloat16))
    return jnp.concatenate(results, axis=1)


BLOCKS = 4
IMAGES = 8
CHUNKS = 2 * IMAGES
LINE = 4
ORDER = (0, 2, 4, 6, 7, 3, 5)


def fits_line(tokens, w_qkv, w_up):
    return (
        lax.axis_size("mp") == LINE
        and lax.axis_size("dp") == IMAGES
        and tokens.shape[0] == PATCHES
        and w_qkv.shape[2] == BLOCKS * HEAD_DIM
        and w_up.shape[1] % (BLOCKS * HEAD_DIM) == 0
    )


def pick(index, table):
    value = table[-1]
    for i in range(len(table) - 2, -1, -1):
        value = jnp.where(index == i, table[i], value)
    return value


def image_of(chunk):
    middle = pick(chunk // 2, ORDER)
    return jnp.where(
        chunk == 0, 0, jnp.where(chunk == 1, 1, jnp.where(chunk == 14, 1, jnp.where(chunk == 15, 0, middle)))
    )


def half_of(chunk):
    edge = jnp.where(chunk < 2, 0, 1)
    return jnp.where((chunk < 2) | (chunk >= CHUNKS - 2), edge, lax.rem(chunk, 2))


def line_kernel(
    tokens, gain, w_heads, w_up, w_attn_out, w_down, out,
    tok, wv, wo, normed, sums, given, sent, got, terms, acc,
    columns, stats_out, stats_in,
    load_sem, stat_send, stat_recv, norm_send, norm_recv,
    sum_send, sum_recv, give_send, give_recv, part_send, part_recv,
):
    d, z = lax.axis_index("dp"), lax.axis_index("mp")
    rows, feat = tok.shape
    width = feat * LINE
    up_block = w_up.shape[1] // BLOCKS
    out_cols = out.shape[1]
    hidden = HEAD_DIM + up_block

    def position(t):
        return jnp.where(t == 1, z, LINE - 1 - z)

    def load(src, dst, k):
        return pltpu.make_async_copy(src, dst, load_sem.at[k])

    loads = [load(tokens, tok, 0)]
    for j in range(BLOCKS):
        loads.append(load(w_heads.at[j], wv.at[j, :, : 3 * HEAD_DIM], 1 + 4 * j))
        loads.append(
            load(w_up.at[:, j * up_block : (j + 1) * up_block], wv.at[j, :, 3 * HEAD_DIM :], 2 + 4 * j)
        )
    for j in range(BLOCKS):
        loads.append(
            load(w_attn_out.at[j * HEAD_DIM : (j + 1) * HEAD_DIM], wo.at[j, :HEAD_DIM], 3 + 4 * j)
        )
        loads.append(load(w_down.at[j * up_block : (j + 1) * up_block], wo.at[j, HEAD_DIM:], 4 + 4 * j))
    for item in loads:
        item.start()

    barrier = pltpu.get_barrier_semaphore()
    for r in range(1, LINE):
        pl.semaphore_signal(barrier, inc=1, device_id=(d, lax.rem(z + r, LINE)), device_id_type=MESH)
    for p in range(1, IMAGES):
        pl.semaphore_signal(barrier, inc=1, device_id=(d ^ p, z), device_id_type=MESH)

    loads[0].wait()
    lane = lax.broadcasted_iota(jnp.int32, (32, HEAD_DIM), 1)

    def measure_rows(i, carry):
        x = tok[pl.ds(i * 32, 32), :].astype(jnp.float32)
        total = jnp.sum(x, axis=1, keepdims=True)
        squares = jnp.sum(x * x, axis=1, keepdims=True)
        columns[0, pl.ds(i * 32, 32), :] = jnp.where(lane < 64, total, squares)
        acc[pl.ds(i * 32, 32), :] = x
        return carry

    lax.fori_loop(0, rows // 32, measure_rows, 0)
    turned = columns[0].T
    stats_out[0:8, :] = turned[0:8]
    stats_out[8:16, :] = turned[64:72]

    pl.semaphore_wait(barrier, LINE - 1 + IMAGES - 1)

    def stat_copy(r):
        return pltpu.make_async_remote_copy(
            src_ref=stats_out, dst_ref=stats_in.at[r - 1], send_sem=stat_send.at[r - 1],
            recv_sem=stat_recv.at[r - 1], device_id=(d, lax.rem(z + r, LINE)), device_id_type=MESH,
        )

    for r in range(1, LINE):
        stat_copy(r).start()
    for r in range(1, LINE):
        stat_copy(r).wait_recv()
    total = stats_out[...] + stats_in[0] + stats_in[1] + stats_in[2]
    mean = total[0:8] / width
    spread = total[8:16] / width - mean * mean
    scale = lax.rsqrt(spread + EPS)
    columns[0] = jnp.concatenate([mean] * (HEAD_DIM // 8), axis=0).T
    columns[1] = jnp.concatenate([scale] * (HEAD_DIM // 8), axis=0).T

    def normalize(i, carry):
        at = pl.ds(i * 32, 32)
        x = acc[at, :]
        scaled = (x - columns[0, at, 0:1]) * columns[1, at, 0:1]
        normed[0, at, :] = (scaled * gain[...]).astype(jnp.bfloat16)
        return carry

    lax.fori_loop(0, rows // 32, normalize, 0)

    def norm_copy(slot, to, offset):
        return pltpu.make_async_remote_copy(
            src_ref=normed.at[slot], dst_ref=normed.at[to], send_sem=norm_send.at[to],
            recv_sem=norm_recv.at[to], device_id=(d ^ offset, z), device_id_type=MESH,
        )

    for p in (1, 2, 4, 6):
        norm_copy(0, p, p).start()

    def sum_copy(t, c):
        return pltpu.make_async_remote_copy(
            src_ref=sums.at[t, c], dst_ref=sums.at[t, c], send_sem=sum_send.at[t, c],
            recv_sem=sum_recv.at[t, c], device_id=(d, lax.rem(z + 2 * t - 1 + LINE, LINE)),
            device_id_type=MESH,
        )

    def give_copy(t, c):
        return pltpu.make_async_remote_copy(
            src_ref=given.at[t, c], dst_ref=given.at[t, c], send_sem=give_send.at[t, c],
            recv_sem=give_recv.at[t, c], device_id=(d, lax.rem(z + 1 - 2 * t + LINE, LINE)),
            device_id_type=MESH,
        )

    def part_copy(p):
        return pltpu.make_async_remote_copy(
            src_ref=sent.at[p - 1], dst_ref=got.at[p - 1], send_sem=part_send.at[p - 1],
            recv_sem=part_recv.at[p - 1], device_id=(d ^ p, z), device_id_type=MESH,
        )

    def prepare(k):
        def one(t, carry):
            c = k - position(t)

            @pl.when((c >= 0) & (c < CHUNKS))
            def _():
                terms[t] = jnp.dot(
                    normed[image_of(c)], wv[2 * t + half_of(c)], preferred_element_type=jnp.float32
                )

            return carry

        lax.fori_loop(0, 2, one, 0)

    for item in loads[1 : 1 + 2 * BLOCKS]:
        item.wait()
    prepare(0)
    for item in loads[1 + 2 * BLOCKS :]:
        item.wait()

    def head_unit(values):
        mean = jnp.mean(values, axis=-1, keepdims=True)
        centered = values - mean
        spread = jnp.mean(centered * centered, axis=-1, keepdims=True)
        return centered * lax.rsqrt(spread + EPS)

    def finish(t, c):
        def column(i):
            value = terms[t, :, i * HEAD_DIM : (i + 1) * HEAD_DIM]
            value = value + sums[t, c, :, i * HEAD_DIM : (i + 1) * HEAD_DIM].astype(jnp.float32)
            return value.astype(jnp.bfloat16)

        query = head_unit(column(0).astype(jnp.float32)) * (1.0 / HEAD_DIM) ** 0.5
        keys = head_unit(column(1).astype(jnp.float32)).astype(jnp.bfloat16)
        scores = lax.dot_general(
            query.astype(jnp.bfloat16), keys, (((1,), (1,)), ((), ())), preferred_element_type=jnp.float32
        )
        weights = jnp.exp(scores)
        probs = (weights / jnp.sum(weights, axis=-1, keepdims=True)).astype(jnp.bfloat16)
        mixed = jnp.dot(probs, column(2), preferred_element_type=jnp.float32)
        given[t, c, :, :HEAD_DIM] = mixed.astype(jnp.bfloat16)
        for i in range(up_block // HEAD_DIM):
            u = column(3 + i).astype(jnp.float32)
            given[t, c, :, (1 + i) * HEAD_DIM : (2 + i) * HEAD_DIM] = jax.nn.gelu(u).astype(jnp.bfloat16)

    def step(k, carry):
        def move_sums(t, carry):
            s = position(t)
            c = k - s

            @pl.when((c >= 0) & (c < CHUNKS))
            def _():
                @pl.when(s > 0)
                def _():
                    sum_copy(t, c).wait_recv()

                @pl.when(s == 0)
                def _():
                    sums[t, c] = terms[t].astype(jnp.bfloat16)
                    sum_copy(t, c).start()

                @pl.when((s > 0) & (s < LINE - 1))
                def _():
                    sums[t, c] = (terms[t] + sums[t, c].astype(jnp.float32)).astype(jnp.bfloat16)
                    sum_copy(t, c).start()

                @pl.when(s == LINE - 1)
                def _():
                    finish(t, c)
                    give_copy(t, c).start()

            return carry

        lax.fori_loop(0, 2, move_sums, 0)

        def move_given(t, carry):
            s = position(t)
            c = k - 2 * (LINE - 1) + s

            @pl.when((c >= 0) & (c < CHUNKS) & (s < LINE - 1))
            def _():
                give_copy(t, c).wait_recv()

                @pl.when(s > 0)
                def _():
                    give_copy(t, c).start()

            return carry

        lax.fori_loop(0, 2, move_given, 0)

        near = jnp.minimum(z, LINE - 1 - z)
        c = k + 1 - near

        @pl.when((c == 1) | (c >= 2) & (c < CHUNKS - 2) & (lax.rem(c, 2) == 0))
        def _():
            p = image_of(c)
            norm_copy(0, p, p).wait_recv()

            @pl.when(lax.rem(p, 2) == 0)
            def _():
                norm_copy(p, p + 1, 1).start()

        prepare(k + 1)

        c = k - 2 * (LINE - 1) + near

        @pl.when((c >= CHUNKS - 2) & (c < CHUNKS) | (c >= 3) & (c < CHUNKS - 2) & (lax.rem(c, 2) == 1))
        def _():
            p = image_of(c)
            first = jnp.where(c == CHUNKS - 2, 1, jnp.where(c == CHUNKS - 1, 0, c - 1))

            def tile(n, carry):
                at = pl.ds(n * 256, 256)
                value = jnp.zeros((rows, 256), jnp.float32)
                for t in range(2):
                    for h, chunk in enumerate((first, c)):
                        value = value + jnp.dot(
                            given[t, chunk], wo[2 * t + h, :, at], preferred_element_type=jnp.float32
                        )

                @pl.when(p == 0)
                def _():
                    acc[:, at] = acc[:, at] + value

                @pl.when(p > 0)
                def _():
                    sent[p - 1, :, at] = value.astype(jnp.bfloat16)

                return carry

            lax.fori_loop(0, out_cols // 256, tile, 0)

            @pl.when(p > 0)
            def _():
                part_copy(p).start()

            @pl.when((c >= 5) & (c < CHUNKS - 2))
            def _():
                collect(pick(c // 2 - 1, ORDER))

        return carry

    def collect(p):
        part_copy(p).wait_recv()

        def add(i, carry):
            at = pl.ds(i * 32, 32)
            acc[at, :] = acc[at, :] + got[p - 1, at, :].astype(jnp.float32)
            return carry

        lax.fori_loop(0, rows // 32, add, 0)

    lax.fori_loop(0, CHUNKS + 2 * (LINE - 1), step, 0)

    part_copy(ORDER[-1]).wait_recv()
    part_copy(1).wait_recv()

    def write(i, carry):
        at = pl.ds(i * 32, 32)
        value = acc[at, :] + got[ORDER[-1] - 1, at, :].astype(jnp.float32)
        out[at, :] = (value + got[0, at, :].astype(jnp.float32)).astype(jnp.bfloat16)
        return carry

    lax.fori_loop(0, rows // 32, write, 0)

    for r in range(1, LINE):
        stat_copy(r).wait_send()
    for p in (1, 2, 4, 6):
        norm_copy(0, p, p).wait_send()
    for p in (2, 4, 6):
        norm_copy(p, p + 1, 1).wait_send()

    def drain(i, carry):
        t, c = i // CHUNKS, lax.rem(i, CHUNKS)
        s = position(t)

        @pl.when(s < LINE - 1)
        def _():
            sum_copy(t, c).wait_send()

        @pl.when(s > 0)
        def _():
            give_copy(t, c).wait_send()

        return carry

    lax.fori_loop(0, 2 * CHUNKS, drain, 0)
    for p in range(1, IMAGES):
        part_copy(p).wait_send()


def on_line(tokens, norm_gain, w_qkv, w_up, w_attn_out, w_down):
    rows, feat = tokens.shape
    units = w_up.shape[1]
    up_block = units // BLOCKS
    out_cols = w_down.shape[1]
    cols = 3 * HEAD_DIM + up_block
    hidden = HEAD_DIM + up_block
    w_heads = w_qkv.reshape(feat, 3, BLOCKS, HEAD_DIM).transpose(2, 0, 1, 3)
    w_heads = w_heads.reshape(BLOCKS, feat, 3 * HEAD_DIM)
    anywhere = pl.BlockSpec(memory_space=pl.ANY)
    inside = pl.BlockSpec(memory_space=pltpu.VMEM)
    dma = pltpu.SemaphoreType.DMA
    return pl.pallas_call(
        line_kernel,
        out_shape=jax.ShapeDtypeStruct((rows, out_cols), jnp.bfloat16),
        in_specs=[anywhere, inside] + [anywhere] * 4,
        out_specs=inside,
        scratch_shapes=[
            pltpu.VMEM((rows, feat), jnp.bfloat16),
            pltpu.VMEM((BLOCKS, feat, cols), jnp.bfloat16),
            pltpu.VMEM((BLOCKS, hidden, out_cols), jnp.bfloat16),
            pltpu.VMEM((IMAGES, rows, feat), jnp.bfloat16),
            pltpu.VMEM((2, CHUNKS, rows, cols), jnp.bfloat16),
            pltpu.VMEM((2, CHUNKS, rows, hidden), jnp.bfloat16),
            pltpu.VMEM((IMAGES - 1, rows, out_cols), jnp.bfloat16),
            pltpu.VMEM((IMAGES - 1, rows, out_cols), jnp.bfloat16),
            pltpu.VMEM((2, rows, cols), jnp.float32),
            pltpu.VMEM((rows, out_cols), jnp.float32),
            pltpu.VMEM((2, rows, HEAD_DIM), jnp.float32),
            pltpu.VMEM((16, rows), jnp.float32),
            pltpu.VMEM((LINE - 1, 16, rows), jnp.float32),
            dma((1 + 4 * BLOCKS,)),
            dma((LINE - 1,)),
            dma((LINE - 1,)),
            dma((IMAGES,)),
            dma((IMAGES,)),
            dma((2, CHUNKS)),
            dma((2, CHUNKS)),
            dma((2, CHUNKS)),
            dma((2, CHUNKS)),
            dma((IMAGES - 1,)),
            dma((IMAGES - 1,)),
        ],
        compiler_params=pltpu.CompilerParams(
            collective_id=0, has_side_effects=True, vmem_limit_bytes=67_000_000
        ),
    )(tokens, norm_gain.reshape(1, feat), w_heads, w_up, w_attn_out, w_down)


def solution(mesh):
    placed = (
        P("dp", "mp"),
        P("mp"),
        P("mp", None, "dp"),
        P("mp", "dp"),
        P("dp", "mp"),
        P("dp", "mp"),
    )
    return jax.shard_map(
        local, mesh=mesh, in_specs=placed, out_specs=P("dp", "mp"), check_vma=False
    )
```

```python
import functools

import jax
import jax.numpy as jnp
from jax import lax
from jax.experimental import pallas as pl
from jax.experimental.pallas import tpu as pltpu
from jax.sharding import PartitionSpec as P

MESH = pl.DeviceIdType.MESH

HEAD_DIM = 128
PATCHES = 256


EPS = 1e-06
UP_SHARES = (1, 2, 2, 1)
FIRST = 1
LAG = 2


def normalize_rows(values, total, squares, gain, width):
    mean = total / width
    spread = squares / width - mean * mean
    scaled = (values - mean[:, None]) * lax.rsqrt(spread + EPS)[:, None]
    return (scaled * gain[None, :]).astype(jnp.bfloat16)


def head_norm(values):
    mean = jnp.mean(values, axis=-1, keepdims=True)
    centered = values - mean
    spread = jnp.mean(centered * centered, axis=-1, keepdims=True)
    return centered * lax.rsqrt(spread + EPS)


def attend(qkv, heads_here):
    rows = qkv.shape[0]
    images = rows // PATCHES
    parts = qkv.reshape(images, PATCHES, 3, heads_here, HEAD_DIM)
    query = (head_norm(parts[:, :, 0].astype(jnp.float32)) * (1.0 / HEAD_DIM) ** 0.5).astype(
        jnp.bfloat16
    )
    keys = head_norm(parts[:, :, 1].astype(jnp.float32)).astype(jnp.bfloat16)
    values = parts[:, :, 2]
    scores = jnp.einsum("iqhd,ikhd->ihqk", query, keys, preferred_element_type=jnp.float32)
    weights = jnp.exp(scores)
    probs = (weights / jnp.sum(weights, axis=-1, keepdims=True)).astype(jnp.bfloat16)
    mixed = jnp.einsum("ihqk,ikhd->iqhd", probs, values, preferred_element_type=jnp.float32)
    return mixed.astype(jnp.bfloat16).reshape(rows, heads_here * HEAD_DIM)


def shift(values, axis, senders, step):
    return lax.ppermute(values, axis, [(i, i + step) for i in senders])


def rows_of(values, block, count):
    return lax.dynamic_slice_in_dim(values, block * count, count, 0)


def add_rounded(*terms):
    total = terms[0].astype(jnp.float32)
    for term in terms[1:]:
        total = total + term.astype(jnp.float32)
    return total.astype(jnp.bfloat16)


class Group:
    def __init__(self, terms, finish, n, me, count):
        self.terms, self.finish, self.n, self.me, self.count = terms, finish, n, me, count
        self.right = self.left = self.own = None
        self.from_left, self.from_right = [], []

    def inputs(self, kind, step):
        n, me, count = self.n, self.me, self.count
        if kind == "scatter":
            send_right = rows_of(self.terms, (me - step - 1) % n, count)
            send_left = rows_of(self.terms, (me + step + 1) % n, count)
            if step:
                send_right = add_rounded(self.right, send_right)
                send_left = add_rounded(self.left, send_left)
            return send_right, send_left
        if step == 0:
            total = add_rounded(rows_of(self.terms, me, count), self.right, self.left)
            self.own = self.finish(total)
            return self.own, self.own
        return self.from_left[-1], self.from_right[-1]

    def move(self, kind, step, send_right, send_left):
        n = self.n
        if kind == "scatter":
            self.right = shift(send_right, "mp", range(step + 1), 1)
            self.left = shift(send_left, "mp", range(n - 1 - step, n), -1)
            return [self.right, self.left]
        self.from_left.append(shift(send_right, "mp", range(step, n - 1), 1))
        self.from_right.append(shift(send_left, "mp", range(1, n - step), -1))
        return [self.from_left[-1], self.from_right[-1]]

    def block(self, r):
        if r == 0:
            return self.own
        near, far = self.from_right[r - 1], self.from_left[self.n - r - 1]
        return jnp.where(self.me + r < self.n, near, far)


def run_line(groups, n):
    if n == 4:
        scatter_at, gather_at, period = [-3, -1, 0], [2, 5, 7], 4
    else:
        scatter_at, gather_at, period = [s - n + 2 for s in range(n - 1)], [2 + s for s in range(n - 1)], n
    slots = {}
    for g, group in enumerate(groups):
        for s in range(n - 1):
            slots.setdefault(g * period + gather_at[s], []).append((group, "gather", s))
            slots.setdefault(g * period + scatter_at[s], []).append((group, "scatter", s))
    history = []
    for at in sorted(slots):
        sends = [pair for group, kind, s in slots[at] for pair in group.inputs(kind, s)]
        if len(history) >= LAG:
            tied = lax.optimization_barrier(tuple(sends) + tuple(history[-LAG]))
            sends = tied[: len(sends)]
        moved = []
        for k, (group, kind, s) in enumerate(slots[at]):
            moved += group.move(kind, s, sends[2 * k], sends[2 * k + 1])
        history.append(moved)


def gather_normed(tokens, stats, n_dp, my_dp, normalize):
    rows, cols = tokens.shape
    if n_dp != 8:
        stats = lax.all_gather(stats, "dp", axis=1, tiled=True)
        return normalize(stats, lax.all_gather(tokens, "dp", axis=0, tiled=True), 0, n_dp)

    def hop(values, offset):
        return lax.ppermute(values, "dp", [(i, i ^ offset) for i in range(n_dp)])

    half = rows // 2
    held = {0: tokens, 2: hop(tokens, 2), 4: hop(tokens, 4)}
    held[1] = hop(tokens, 1)
    stats, held[2], held[4] = lax.optimization_barrier((stats, held[2], held[4]))
    stats = lax.all_gather(stats, "dp", axis=1, tiled=True)
    upper, lower = hop(held[2][:half], 4), hop(held[4][half:], 2)
    held[6] = jnp.concatenate([upper, lower])
    for offset in (2, 4, 6):
        held[offset ^ 1] = hop(held[offset], 1)
    result = jnp.zeros((n_dp * rows, cols), jnp.bfloat16)
    for offset in (0, 1, 2, 3, 4, 5, 6, 7):
        index = my_dp ^ offset
        result = lax.dynamic_update_slice_in_dim(
            result, normalize(stats, held[offset], index, 1), index * rows, 0
        )
    return result


def swap(values, bit, mine, dim, size):
    keep = lax.dynamic_index_in_dim(values, mine, dim, keepdims=False)
    give = lax.dynamic_index_in_dim(values, 1 - mine, dim, keepdims=False)
    got = lax.ppermute(give, "dp", [(i, i ^ (1 << bit)) for i in range(size)])
    return keep, got


def local(tokens, norm_gain, w_qkv, w_up, w_attn_out, w_down):
    if fits_line(tokens, w_qkv, w_up):
        return on_line(tokens, norm_gain, w_qkv, w_up, w_attn_out, w_down)
    n_mp, n_dp = lax.axis_size("mp"), lax.axis_size("dp")
    me, my_dp = lax.axis_index("mp"), lax.axis_index("dp")
    rows_here, feat_here = tokens.shape
    head_cols = w_qkv.shape[2]
    heads_here = head_cols // HEAD_DIM
    units = w_up.shape[1]
    width = feat_here * n_mp
    count = rows_here * n_dp // n_mp
    tokens_f = tokens.astype(jnp.float32)

    stats = lax.psum(
        jnp.stack([jnp.sum(tokens_f, axis=1), jnp.sum(tokens_f * tokens_f, axis=1)]), "mp"
    )

    def normalize(stats, block, index, many):
        here = lax.dynamic_slice_in_dim(stats, index * rows_here, many * rows_here, 1)
        return normalize_rows(block.astype(jnp.float32), here[0], here[1], norm_gain, width)

    normed = gather_normed(tokens, stats, n_dp, my_dp, normalize)

    halves = 2 if heads_here % 2 == 0 else 1
    group_heads = heads_here // halves
    group_cols = group_heads * HEAD_DIM

    def attention(projected):
        return attend(projected.reshape(count, 3, group_cols), group_heads)

    def activation(projected):
        return jax.nn.gelu(projected.astype(jnp.float32)).astype(jnp.bfloat16)

    heads = [("heads", g * group_cols, group_cols) for g in range(halves)]
    ups, first = [], 0
    for share in UP_SHARES:
        ups.append(("up", first, units * share // sum(UP_SHARES)))
        first += units * share // sum(UP_SHARES)
    groups = []
    weights_out = []
    for kind, start, size in ups[:FIRST] + heads + ups[FIRST:]:
        if kind == "heads":
            weight = w_qkv[:, :, start : start + size].reshape(feat_here, 3 * size)
            finish, weight_out = attention, w_attn_out[start : start + size]
        else:
            weight = w_up[:, start : start + size]
            finish, weight_out = activation, w_down[start : start + size]
        terms = jnp.dot(normed, weight, preferred_element_type=jnp.float32).astype(jnp.bfloat16)
        groups.append(Group(terms, finish, n_mp, me, count))
        weights_out.append(weight_out)
    run_line(groups, n_mp)

    order = sorted(range(n_mp), key=lambda r: min(r, n_mp - r))
    out_cols = w_down.shape[1]
    bits = n_dp.bit_length() - 1
    core = my_dp % 2
    pairs = count // rows_here // 2
    kept = jnp.zeros((n_mp * pairs, rows_here, out_cols), jnp.bfloat16)
    for r in order:
        block = sum(
            jnp.dot(group.block(r), weight, preferred_element_type=jnp.float32)
            for group, weight in zip(groups, weights_out)
        ).astype(jnp.bfloat16)
        block = block.reshape(pairs, 2, rows_here, out_cols)
        keep, got = swap(block, 0, core, 1, n_dp)
        kept = lax.dynamic_update_slice_in_dim(
            kept, add_rounded(keep, got), (me + r) % n_mp * pairs, 0
        )
    rest = list(range(1, bits))
    half = out_cols // 2
    results = []
    for part, bit_order in enumerate((rest, rest[::-1])):
        values = kept[:, :, part * half : (part + 1) * half].reshape(
            [2] * len(rest) + [rows_here, half]
        )
        left_bits = list(rest)
        base = tokens_f[:, part * half : (part + 1) * half]
        for bit in bit_order:
            dim = len(left_bits) - 1 - left_bits.index(bit)
            keep, got = swap(values, bit, (my_dp >> bit) % 2, dim, n_dp)
            left_bits.remove(bit)
            if left_bits:
                values = add_rounded(keep, got)
            else:
                total = base + (keep.astype(jnp.float32) + got.astype(jnp.float32))
                results.append(total.astype(jnp.bfloat16))
    return jnp.concatenate(results, axis=1)


BLOCKS = 4
IMAGES = 8
CHUNKS = 2 * IMAGES
LINE = 4
PIECES = 2
ORDER = (0, 2, 4, 6, 7, 3, 5, 1, 0)


def fits_line(tokens, w_qkv, w_up):
    return (
        lax.axis_size("mp") == LINE
        and lax.axis_size("dp") == IMAGES
        and tokens.shape[0] == PATCHES
        and w_qkv.shape[2] == BLOCKS * HEAD_DIM
        and w_up.shape[1] % (BLOCKS * HEAD_DIM) == 0
    )


def pick(index, table):
    value = table[-1]
    for i in range(len(table) - 2, -1, -1):
        value = jnp.where(index == i, table[i], value)
    return value


def image_of(pair, core):
    offset = pick(pair, ORDER)
    crossed = pick(offset, (0, 1, 4, 5, 2, 3, 6, 7))
    return jnp.where(core == 1, crossed, offset)


def line_kernel(
    tokens, gain, w_heads, w_up, w_attn_out, w_down, out,
    tok, wv, wo, normed, sums, given, sent, got, terms, acc,
    columns, stats_out, stats_in,
    load_sem, stat_send, stat_recv, norm_send, norm_recv,
    sum_send, sum_recv, give_send, give_recv, part_send, part_recv,
):
    d, z = lax.axis_index("dp"), lax.axis_index("mp")
    core = lax.rem(d, 2)
    rows, feat = tok.shape
    width = feat * LINE
    up_block = w_up.shape[1] // BLOCKS
    out_cols = out.shape[1]
    hidden = HEAD_DIM + up_block

    def position(t):
        return jnp.where(t == 1, z, LINE - 1 - z)

    def load(src, dst, k):
        return pltpu.make_async_copy(src, dst, load_sem.at[k])

    loads = [load(tokens, tok, 0)]
    for j in range(BLOCKS):
        for i in range(3):
            loads.append(
                load(
                    w_heads.at[i, :, j * HEAD_DIM : (j + 1) * HEAD_DIM],
                    wv.at[j, :, i * HEAD_DIM : (i + 1) * HEAD_DIM],
                    1 + 6 * j + i,
                )
            )
        loads.append(
            load(w_up.at[:, j * up_block : (j + 1) * up_block], wv.at[j, :, 3 * HEAD_DIM :], 4 + 6 * j)
        )
    for j in range(BLOCKS):
        loads.append(
            load(w_attn_out.at[j * HEAD_DIM : (j + 1) * HEAD_DIM], wo.at[j, :HEAD_DIM], 5 + 6 * j)
        )
        loads.append(load(w_down.at[j * up_block : (j + 1) * up_block], wo.at[j, HEAD_DIM:], 6 + 6 * j))
    for item in loads:
        item.start()

    barrier = pltpu.get_barrier_semaphore()
    for r in range(1, LINE):
        pl.semaphore_signal(barrier, inc=1, device_id=(d, lax.rem(z + r, LINE)), device_id_type=MESH)
    for p in range(1, IMAGES):
        pl.semaphore_signal(barrier, inc=1, device_id=(d ^ p, z), device_id_type=MESH)

    loads[0].wait()
    lane = lax.broadcasted_iota(jnp.int32, (32, HEAD_DIM), 1)

    def measure_rows(i, carry):
        x = tok[pl.ds(i * 32, 32), :].astype(jnp.float32)
        total = jnp.sum(x, axis=1, keepdims=True)
        squares = jnp.sum(x * x, axis=1, keepdims=True)
        columns[0, pl.ds(i * 32, 32), :] = jnp.where(lane < 64, total, squares)
        acc[pl.ds(i * 32, 32), :] = x
        return carry

    lax.fori_loop(0, rows // 32, measure_rows, 0)
    turned = columns[0].T
    stats_out[0:8, :] = turned[0:8]
    stats_out[8:16, :] = turned[64:72]

    pl.semaphore_wait(barrier, LINE - 1 + IMAGES - 1)

    def stat_copy(r):
        return pltpu.make_async_remote_copy(
            src_ref=stats_out, dst_ref=stats_in.at[r - 1], send_sem=stat_send.at[r - 1],
            recv_sem=stat_recv.at[r - 1], device_id=(d, lax.rem(z + r, LINE)), device_id_type=MESH,
        )

    for r in range(1, LINE):
        stat_copy(r).start()
    for r in range(1, LINE):
        stat_copy(r).wait_recv()
    total = stats_out[...] + stats_in[0] + stats_in[1] + stats_in[2]
    mean = total[0:8] / width
    spread = total[8:16] / width - mean * mean
    scale = lax.rsqrt(spread + EPS)
    columns[0] = jnp.concatenate([mean] * (HEAD_DIM // 8), axis=0).T
    columns[1] = jnp.concatenate([scale] * (HEAD_DIM // 8), axis=0).T

    def normalize(i, carry):
        at = pl.ds(i * 32, 32)
        x = acc[at, :]
        scaled = (x - columns[0, at, 0:1]) * columns[1, at, 0:1]
        normed[0, at, :] = (scaled * gain[...][None, :]).astype(jnp.bfloat16)
        return carry

    lax.fori_loop(0, rows // 32, normalize, 0)

    piece = rows // PIECES

    def norm_copy(slot, to, offset, i):
        at = pl.ds(i * piece, piece)
        return pltpu.make_async_remote_copy(
            src_ref=normed.at[slot, at], dst_ref=normed.at[to, at], send_sem=norm_send.at[to],
            recv_sem=norm_recv.at[to, i], device_id=(d ^ offset, z), device_id_type=MESH,
        )

    near, far = image_of(1, core), image_of(2, core)
    for p in (near, 1):
        for i in range(PIECES):
            norm_copy(0, p, p, i).start()


    def ready(c, i):
        @pl.when((lax.rem(c, 2) == 1) & (c < CHUNKS - 1))
        def _():
            p = image_of((c + 1) // 2, core)
            norm_copy(0, p, p, i).wait_recv()

            @pl.when(lax.rem(p, 2) == 0)
            def _():
                norm_copy(p, p + 1, 1, i).start()

    def sum_copy(t, c, i):
        part = sums.at[t, c, i * piece : (i + 1) * piece]
        return pltpu.make_async_remote_copy(
            src_ref=part, dst_ref=part, send_sem=sum_send.at[t],
            recv_sem=sum_recv.at[t, c, i], device_id=(d, lax.rem(z + 2 * t - 1 + LINE, LINE)),
            device_id_type=MESH,
        )

    def give_copy(t, c, i):
        part = given.at[t, c, i * piece : (i + 1) * piece]
        return pltpu.make_async_remote_copy(
            src_ref=part, dst_ref=part, send_sem=give_send.at[t],
            recv_sem=give_recv.at[t, c, i], device_id=(d, lax.rem(z + 1 - 2 * t + LINE, LINE)),
            device_id_type=MESH,
        )

    def part_copy(p):
        return pltpu.make_async_remote_copy(
            src_ref=sent.at[p - 1], dst_ref=got.at[p - 1], send_sem=part_send.at[p - 1],
            recv_sem=part_recv.at[p - 1], device_id=(d ^ p, z), device_id_type=MESH,
        )

    def term(c, t, at):
        return jnp.dot(
            normed[image_of((c + 1) // 2, core), at, :], wv[2 * t + lax.rem(c + 1, 2)], preferred_element_type=jnp.float32
        )

    def prepare(k):
        def one(t, carry):
            s = position(t)
            c = k - s

            @pl.when((s > 0) & (c >= 0) & (c < CHUNKS))
            def _():
                @pl.when(s == 1)
                def _():
                    for i in range(PIECES):
                        ready(c, i)

                terms[t] = term(c, t, slice(None))

            return carry

        lax.fori_loop(0, 2, one, 0)

    for item in loads[1:]:
        item.wait()

    def head_unit(values):
        mean = jnp.mean(values, axis=-1, keepdims=True)
        centered = values - mean
        spread = jnp.mean(centered * centered, axis=-1, keepdims=True)
        return centered * lax.rsqrt(spread + EPS)

    def finish(t, c):
        def column(i):
            value = terms[t, :, i * HEAD_DIM : (i + 1) * HEAD_DIM]
            value = value + sums[t, c, :, i * HEAD_DIM : (i + 1) * HEAD_DIM].astype(jnp.float32)
            return value.astype(jnp.bfloat16)

        query = head_unit(column(0).astype(jnp.float32)) * (1.0 / HEAD_DIM) ** 0.5
        keys = head_unit(column(1).astype(jnp.float32)).astype(jnp.bfloat16)
        scores = lax.dot_general(
            query.astype(jnp.bfloat16), keys, (((1,), (1,)), ((), ())), preferred_element_type=jnp.float32
        )
        weights = jnp.exp(scores)
        probs = (weights / jnp.sum(weights, axis=-1, keepdims=True)).astype(jnp.bfloat16)
        mixed = jnp.dot(probs, column(2), preferred_element_type=jnp.float32)
        given[t, c, :, :HEAD_DIM] = mixed.astype(jnp.bfloat16)
        for i in range(up_block // HEAD_DIM):
            u = column(3 + i).astype(jnp.float32)
            given[t, c, :, (1 + i) * HEAD_DIM : (2 + i) * HEAD_DIM] = jax.nn.gelu(u).astype(jnp.bfloat16)

    def sent_from(whole, sem):
        pltpu.make_async_remote_copy(
            src_ref=whole, dst_ref=whole, send_sem=sem, recv_sem=sem,
            device_id=(d, lax.rem(z + 1, LINE)), device_id_type=MESH,
        ).wait_send()

    def step(k, carry):
        def stream(n):
            return jnp.where(z < LINE // 2, 1 - n, n)

        def move_sums(n, carry, i):
            t = stream(n)
            s = position(t)
            c = k - s

            @pl.when((c >= 0) & (c < CHUNKS))
            def _():
                at = pl.ds(i * piece, piece)

                @pl.when(s > 0)
                def _():
                    sum_copy(t, c, i).wait_recv()

                @pl.when(s == 0)
                def _():
                    ready(c, i)
                    sums[t, c, at, :] = term(c, t, at).astype(jnp.bfloat16)
                    sum_copy(t, c, i).start()

                @pl.when((s > 0) & (s < LINE - 1))
                def _():
                    value = terms[t, at, :] + sums[t, c, at, :].astype(jnp.float32)
                    sums[t, c, at, :] = value.astype(jnp.bfloat16)
                    sum_copy(t, c, i).start()

                if i == PIECES - 1:

                    @pl.when(s == LINE - 1)
                    def _():
                        finish(t, c)
                        for j in range(PIECES):
                            give_copy(t, c, j).start()

            return carry

        for i in range(PIECES):
            lax.fori_loop(0, 2, functools.partial(move_sums, i=i), 0)

        def move_given(n, carry):
            t = stream(n)
            s = position(t)
            c = k - 2 * (LINE - 1) + s

            @pl.when((c >= 0) & (c < CHUNKS) & (s < LINE - 1))
            def _():
                for i in range(PIECES):
                    give_copy(t, c, i).wait_recv()

                    @pl.when(s > 0)
                    def _():
                        give_copy(t, c, i).start()

            return carry

        lax.fori_loop(0, 2, move_given, 0)
        @pl.when(k == 1)
        def _():
            sent_from(normed.at[0], norm_send.at[near])
            for i in range(PIECES):
                norm_copy(0, far, far, i).start()

        @pl.when(k == 3)
        def _():
            for i in range(PIECES):
                norm_copy(0, 6, 6, i).start()

        prepare(k + 1)

        c = k - 2 * (LINE - 1) + jnp.minimum(z, LINE - 1 - z)

        def tiles(work):
            def one(n, carry):
                work(pl.ds(n * 256, 256))
                return carry

            lax.fori_loop(0, out_cols // 256, one, 0)

        @pl.when((c == 0) | (c == CHUNKS - 1))
        def _():
            h = lax.rem(c + 1, 2)

            def own(at):
                value = acc[:, at]
                for t in range(2):
                    value = value + jnp.dot(
                        given[t, c], wo[2 * t + h, :, at], preferred_element_type=jnp.float32
                    )
                acc[:, at] = value

            tiles(own)

        @pl.when((c >= 2) & (c < CHUNKS) & (lax.rem(c, 2) == 0))
        def _():
            p = image_of(c // 2, core)

            def other(at):
                value = jnp.zeros((rows, 256), jnp.float32)
                for t in range(2):
                    for h, chunk in enumerate((c - 1, c)):
                        value = value + jnp.dot(
                            given[t, chunk], wo[2 * t + h, :, at], preferred_element_type=jnp.float32
                        )
                sent[p - 1, :, at] = value.astype(jnp.bfloat16)

            tiles(other)
            part_copy(p).start()

            @pl.when((c >= 4) & (c < CHUNKS - 2))
            def _():
                collect(c // 2 - 1)

        return carry

    def arrival(pair):
        p = pick(pair, ORDER)
        return image_of(pair, jnp.where(lax.rem(p, 2) == 1, 1 - core, core))

    def collect(pair):
        p = arrival(pair)
        part_copy(p).wait_recv()

        def add(i, carry):
            at = pl.ds(i * 32, 32)
            acc[at, :] = acc[at, :] + got[p - 1, at, :].astype(jnp.float32)
            return carry

        lax.fori_loop(0, rows // 32, add, 0)

    lax.fori_loop(0, CHUNKS + 2 * (LINE - 1), step, 0)

    last = arrival(CHUNKS // 2 - 2)
    part_copy(last).wait_recv()
    part_copy(1).wait_recv()

    def write(i, carry):
        at = pl.ds(i * 32, 32)
        value = acc[at, :] + got[last - 1, at, :].astype(jnp.float32)
        tok[at, :] = (value + got[0, at, :].astype(jnp.float32)).astype(jnp.bfloat16)
        return carry

    lax.fori_loop(0, rows // 32, write, 0)
    store = pltpu.make_async_copy(tok, out, load_sem.at[0])
    store.start()

    for r in range(1, LINE):
        stat_copy(r).wait_send()
    for p in (1, far, 6):
        sent_from(normed.at[0], norm_send.at[p])
    for p in (2, 4, 6):
        sent_from(normed.at[p], norm_send.at[p + 1])

    for t in range(2):

        @pl.when(position(t) < LINE - 1)
        def _():
            sent_from(sums.at[t], sum_send.at[t])

        @pl.when(position(t) > 0)
        def _():
            sent_from(given.at[t], give_send.at[t])

    for p in range(1, IMAGES):
        part_copy(p).wait_send()
    store.wait()


def on_line(tokens, norm_gain, w_qkv, w_up, w_attn_out, w_down):
    rows, feat = tokens.shape
    units = w_up.shape[1]
    up_block = units // BLOCKS
    out_cols = w_down.shape[1]
    cols = 3 * HEAD_DIM + up_block
    hidden = HEAD_DIM + up_block
    w_heads = w_qkv.transpose(1, 0, 2)
    anywhere = pl.BlockSpec(memory_space=pl.ANY)
    inside = pl.BlockSpec(memory_space=pltpu.VMEM)
    dma = pltpu.SemaphoreType.DMA
    return pl.pallas_call(
        line_kernel,
        out_shape=jax.ShapeDtypeStruct((rows, out_cols), jnp.bfloat16),
        in_specs=[anywhere, inside] + [anywhere] * 4,
        out_specs=anywhere,
        scratch_shapes=[
            pltpu.VMEM((rows, feat), jnp.bfloat16),
            pltpu.VMEM((BLOCKS, feat, cols), jnp.bfloat16),
            pltpu.VMEM((BLOCKS, hidden, out_cols), jnp.bfloat16),
            pltpu.VMEM((IMAGES, rows, feat), jnp.bfloat16),
            pltpu.VMEM((2, CHUNKS, rows, cols), jnp.bfloat16),
            pltpu.VMEM((2, CHUNKS, rows, hidden), jnp.bfloat16),
            pltpu.VMEM((IMAGES - 1, rows, out_cols), jnp.bfloat16),
            pltpu.VMEM((IMAGES - 1, rows, out_cols), jnp.bfloat16),
            pltpu.VMEM((2, rows, cols), jnp.float32),
            pltpu.VMEM((rows, out_cols), jnp.float32),
            pltpu.VMEM((2, rows, HEAD_DIM), jnp.float32),
            pltpu.VMEM((16, rows), jnp.float32),
            pltpu.VMEM((LINE - 1, 16, rows), jnp.float32),
            dma((1 + 6 * BLOCKS,)),
            dma((LINE - 1,)),
            dma((LINE - 1,)),
            dma((IMAGES,)),
            dma((IMAGES, PIECES)),
            dma((2,)),
            dma((2, CHUNKS, PIECES)),
            dma((2,)),
            dma((2, CHUNKS, PIECES)),
            dma((IMAGES - 1,)),
            dma((IMAGES - 1,)),
        ],
        compiler_params=pltpu.CompilerParams(
            collective_id=0, has_side_effects=True, vmem_limit_bytes=67_000_000
        ),
    )(tokens, norm_gain, w_heads, w_up, w_attn_out, w_down)


def solution(mesh):
    placed = (
        P("dp", "mp"),
        P("mp"),
        P("mp", None, "dp"),
        P("mp", "dp"),
        P("dp", "mp"),
        P("dp", "mp"),
    )
    return jax.shard_map(
        local, mesh=mesh, in_specs=placed, out_specs=P("dp", "mp"), check_vma=False
    )
```

```python
import functools

import jax
import jax.numpy as jnp
from jax import lax
from jax.experimental import pallas as pl
from jax.experimental.pallas import tpu as pltpu
from jax.sharding import PartitionSpec as P

MESH = pl.DeviceIdType.MESH

HEAD_DIM = 128
PATCHES = 256


EPS = 1e-06
UP_SHARES = (1, 2, 2, 1)
FIRST = 1
LAG = 2


def normalize_rows(values, total, squares, gain, width):
    mean = total / width
    spread = squares / width - mean * mean
    scaled = (values - mean[:, None]) * lax.rsqrt(spread + EPS)[:, None]
    return (scaled * gain[None, :]).astype(jnp.bfloat16)


def head_norm(values):
    mean = jnp.mean(values, axis=-1, keepdims=True)
    centered = values - mean
    spread = jnp.mean(centered * centered, axis=-1, keepdims=True)
    return centered * lax.rsqrt(spread + EPS)


def attend(qkv, heads_here):
    rows = qkv.shape[0]
    images = rows // PATCHES
    parts = qkv.reshape(images, PATCHES, 3, heads_here, HEAD_DIM)
    query = (head_norm(parts[:, :, 0].astype(jnp.float32)) * (1.0 / HEAD_DIM) ** 0.5).astype(
        jnp.bfloat16
    )
    keys = head_norm(parts[:, :, 1].astype(jnp.float32)).astype(jnp.bfloat16)
    values = parts[:, :, 2]
    scores = jnp.einsum("iqhd,ikhd->ihqk", query, keys, preferred_element_type=jnp.float32)
    weights = jnp.exp(scores)
    probs = (weights / jnp.sum(weights, axis=-1, keepdims=True)).astype(jnp.bfloat16)
    mixed = jnp.einsum("ihqk,ikhd->iqhd", probs, values, preferred_element_type=jnp.float32)
    return mixed.astype(jnp.bfloat16).reshape(rows, heads_here * HEAD_DIM)


def shift(values, axis, senders, step):
    return lax.ppermute(values, axis, [(i, i + step) for i in senders])


def rows_of(values, block, count):
    return lax.dynamic_slice_in_dim(values, block * count, count, 0)


def add_rounded(*terms):
    total = terms[0].astype(jnp.float32)
    for term in terms[1:]:
        total = total + term.astype(jnp.float32)
    return total.astype(jnp.bfloat16)


class Group:
    def __init__(self, terms, finish, n, me, count):
        self.terms, self.finish, self.n, self.me, self.count = terms, finish, n, me, count
        self.right = self.left = self.own = None
        self.from_left, self.from_right = [], []

    def inputs(self, kind, step):
        n, me, count = self.n, self.me, self.count
        if kind == "scatter":
            send_right = rows_of(self.terms, (me - step - 1) % n, count)
            send_left = rows_of(self.terms, (me + step + 1) % n, count)
            if step:
                send_right = add_rounded(self.right, send_right)
                send_left = add_rounded(self.left, send_left)
            return send_right, send_left
        if step == 0:
            total = add_rounded(rows_of(self.terms, me, count), self.right, self.left)
            self.own = self.finish(total)
            return self.own, self.own
        return self.from_left[-1], self.from_right[-1]

    def move(self, kind, step, send_right, send_left):
        n = self.n
        if kind == "scatter":
            self.right = shift(send_right, "mp", range(step + 1), 1)
            self.left = shift(send_left, "mp", range(n - 1 - step, n), -1)
            return [self.right, self.left]
        self.from_left.append(shift(send_right, "mp", range(step, n - 1), 1))
        self.from_right.append(shift(send_left, "mp", range(1, n - step), -1))
        return [self.from_left[-1], self.from_right[-1]]

    def block(self, r):
        if r == 0:
            return self.own
        near, far = self.from_right[r - 1], self.from_left[self.n - r - 1]
        return jnp.where(self.me + r < self.n, near, far)


def run_line(groups, n):
    if n == 4:
        scatter_at, gather_at, period = [-3, -1, 0], [2, 5, 7], 4
    else:
        scatter_at, gather_at, period = [s - n + 2 for s in range(n - 1)], [2 + s for s in range(n - 1)], n
    slots = {}
    for g, group in enumerate(groups):
        for s in range(n - 1):
            slots.setdefault(g * period + gather_at[s], []).append((group, "gather", s))
            slots.setdefault(g * period + scatter_at[s], []).append((group, "scatter", s))
    history = []
    for at in sorted(slots):
        sends = [pair for group, kind, s in slots[at] for pair in group.inputs(kind, s)]
        if len(history) >= LAG:
            tied = lax.optimization_barrier(tuple(sends) + tuple(history[-LAG]))
            sends = tied[: len(sends)]
        moved = []
        for k, (group, kind, s) in enumerate(slots[at]):
            moved += group.move(kind, s, sends[2 * k], sends[2 * k + 1])
        history.append(moved)


def gather_normed(tokens, stats, n_dp, my_dp, normalize):
    rows, cols = tokens.shape
    if n_dp != 8:
        stats = lax.all_gather(stats, "dp", axis=1, tiled=True)
        return normalize(stats, lax.all_gather(tokens, "dp", axis=0, tiled=True), 0, n_dp)

    def hop(values, offset):
        return lax.ppermute(values, "dp", [(i, i ^ offset) for i in range(n_dp)])

    half = rows // 2
    held = {0: tokens, 2: hop(tokens, 2), 4: hop(tokens, 4)}
    held[1] = hop(tokens, 1)
    stats, held[2], held[4] = lax.optimization_barrier((stats, held[2], held[4]))
    stats = lax.all_gather(stats, "dp", axis=1, tiled=True)
    upper, lower = hop(held[2][:half], 4), hop(held[4][half:], 2)
    held[6] = jnp.concatenate([upper, lower])
    for offset in (2, 4, 6):
        held[offset ^ 1] = hop(held[offset], 1)
    result = jnp.zeros((n_dp * rows, cols), jnp.bfloat16)
    for offset in (0, 1, 2, 3, 4, 5, 6, 7):
        index = my_dp ^ offset
        result = lax.dynamic_update_slice_in_dim(
            result, normalize(stats, held[offset], index, 1), index * rows, 0
        )
    return result


def swap(values, bit, mine, dim, size):
    keep = lax.dynamic_index_in_dim(values, mine, dim, keepdims=False)
    give = lax.dynamic_index_in_dim(values, 1 - mine, dim, keepdims=False)
    got = lax.ppermute(give, "dp", [(i, i ^ (1 << bit)) for i in range(size)])
    return keep, got


def local(tokens, norm_gain, w_qkv, w_up, w_attn_out, w_down):
    if fits_line(tokens, w_qkv, w_up):
        return on_line(tokens, norm_gain, w_qkv, w_up, w_attn_out, w_down)
    n_mp, n_dp = lax.axis_size("mp"), lax.axis_size("dp")
    me, my_dp = lax.axis_index("mp"), lax.axis_index("dp")
    rows_here, feat_here = tokens.shape
    head_cols = w_qkv.shape[2]
    heads_here = head_cols // HEAD_DIM
    units = w_up.shape[1]
    width = feat_here * n_mp
    count = rows_here * n_dp // n_mp
    tokens_f = tokens.astype(jnp.float32)

    stats = lax.psum(
        jnp.stack([jnp.sum(tokens_f, axis=1), jnp.sum(tokens_f * tokens_f, axis=1)]), "mp"
    )

    def normalize(stats, block, index, many):
        here = lax.dynamic_slice_in_dim(stats, index * rows_here, many * rows_here, 1)
        return normalize_rows(block.astype(jnp.float32), here[0], here[1], norm_gain, width)

    normed = gather_normed(tokens, stats, n_dp, my_dp, normalize)

    halves = 2 if heads_here % 2 == 0 else 1
    group_heads = heads_here // halves
    group_cols = group_heads * HEAD_DIM

    def attention(projected):
        return attend(projected.reshape(count, 3, group_cols), group_heads)

    def activation(projected):
        return jax.nn.gelu(projected.astype(jnp.float32)).astype(jnp.bfloat16)

    heads = [("heads", g * group_cols, group_cols) for g in range(halves)]
    ups, first = [], 0
    for share in UP_SHARES:
        ups.append(("up", first, units * share // sum(UP_SHARES)))
        first += units * share // sum(UP_SHARES)
    groups = []
    weights_out = []
    for kind, start, size in ups[:FIRST] + heads + ups[FIRST:]:
        if kind == "heads":
            weight = w_qkv[:, :, start : start + size].reshape(feat_here, 3 * size)
            finish, weight_out = attention, w_attn_out[start : start + size]
        else:
            weight = w_up[:, start : start + size]
            finish, weight_out = activation, w_down[start : start + size]
        terms = jnp.dot(normed, weight, preferred_element_type=jnp.float32).astype(jnp.bfloat16)
        groups.append(Group(terms, finish, n_mp, me, count))
        weights_out.append(weight_out)
    run_line(groups, n_mp)

    order = sorted(range(n_mp), key=lambda r: min(r, n_mp - r))
    out_cols = w_down.shape[1]
    bits = n_dp.bit_length() - 1
    core = my_dp % 2
    pairs = count // rows_here // 2
    kept = jnp.zeros((n_mp * pairs, rows_here, out_cols), jnp.bfloat16)
    for r in order:
        block = sum(
            jnp.dot(group.block(r), weight, preferred_element_type=jnp.float32)
            for group, weight in zip(groups, weights_out)
        ).astype(jnp.bfloat16)
        block = block.reshape(pairs, 2, rows_here, out_cols)
        keep, got = swap(block, 0, core, 1, n_dp)
        kept = lax.dynamic_update_slice_in_dim(
            kept, add_rounded(keep, got), (me + r) % n_mp * pairs, 0
        )
    rest = list(range(1, bits))
    half = out_cols // 2
    results = []
    for part, bit_order in enumerate((rest, rest[::-1])):
        values = kept[:, :, part * half : (part + 1) * half].reshape(
            [2] * len(rest) + [rows_here, half]
        )
        left_bits = list(rest)
        base = tokens_f[:, part * half : (part + 1) * half]
        for bit in bit_order:
            dim = len(left_bits) - 1 - left_bits.index(bit)
            keep, got = swap(values, bit, (my_dp >> bit) % 2, dim, n_dp)
            left_bits.remove(bit)
            if left_bits:
                values = add_rounded(keep, got)
            else:
                total = base + (keep.astype(jnp.float32) + got.astype(jnp.float32))
                results.append(total.astype(jnp.bfloat16))
    return jnp.concatenate(results, axis=1)


BLOCKS = 4
IMAGES = 8
CHUNKS = 2 * IMAGES
LINE = 4
PIECES = 2
TURNS = 8
UNROLL = 4
ORDER = (0, 2, 4, 6, 7, 3, 5, 1, 0)


def fits_line(tokens, w_qkv, w_up):
    return (
        lax.axis_size("mp") == LINE
        and lax.axis_size("dp") == IMAGES
        and tokens.shape[0] == PATCHES
        and w_qkv.shape[2] == BLOCKS * HEAD_DIM
        and w_up.shape[1] % (BLOCKS * HEAD_DIM) == 0
    )


def pick(index, table):
    value = table[-1]
    for i in range(len(table) - 2, -1, -1):
        value = jnp.where(index == i, table[i], value)
    return value


def image_of(pair, core):
    offset = pick(pair, ORDER)
    crossed = pick(offset, (0, 1, 4, 5, 2, 3, 6, 7))
    return jnp.where(core == 1, crossed, offset)


def line_kernel(
    tokens, gain, w_heads, w_up, w_attn_out, w_down, out,
    tok, wv, wo, normed, sums, given, sent, got, terms, acc,
    columns, stats_out, stats_in,
    load_sem, stat_send, stat_recv, norm_send, norm_recv,
    sum_send, sum_recv, give_send, give_recv, part_send, part_recv,
):
    d, z = lax.axis_index("dp"), lax.axis_index("mp")
    core = lax.rem(d, 2)
    rows, feat = tok.shape
    width = feat * LINE
    up_block = w_up.shape[1] // BLOCKS
    out_cols = out.shape[1]
    hidden = HEAD_DIM + up_block

    def position(t):
        return jnp.where(t == 1, z, LINE - 1 - z)

    def load(src, dst, k):
        return pltpu.make_async_copy(src, dst, load_sem.at[k])

    loads = [load(tokens, tok, 0)]
    for j in range(BLOCKS):
        for i in range(3):
            loads.append(
                load(
                    w_heads.at[i, :, j * HEAD_DIM : (j + 1) * HEAD_DIM],
                    wv.at[j, :, i * HEAD_DIM : (i + 1) * HEAD_DIM],
                    1 + 6 * j + i,
                )
            )
        loads.append(
            load(w_up.at[:, j * up_block : (j + 1) * up_block], wv.at[j, :, 3 * HEAD_DIM :], 4 + 6 * j)
        )
    for j in range(BLOCKS):
        loads.append(
            load(w_attn_out.at[j * HEAD_DIM : (j + 1) * HEAD_DIM], wo.at[j, :HEAD_DIM], 5 + 6 * j)
        )
        loads.append(load(w_down.at[j * up_block : (j + 1) * up_block], wo.at[j, HEAD_DIM:], 6 + 6 * j))
    barrier = pltpu.get_barrier_semaphore()
    for r in range(1, LINE):
        pl.semaphore_signal(barrier, inc=1, device_id=(d, lax.rem(z + r, LINE)), device_id_type=MESH)
    loads[0].start()
    for p in range(1, IMAGES):
        pl.semaphore_signal(barrier, inc=1, device_id=(d ^ p, z), device_id_type=MESH)
    for item in loads[1:]:
        item.start()

    loads[0].wait()
    lane = lax.broadcasted_iota(jnp.int32, (32, HEAD_DIM), 1)

    def measure_rows(i, carry):
        x = tok[pl.ds(i * 32, 32), :].astype(jnp.float32)
        total = jnp.sum(x, axis=1, keepdims=True)
        squares = jnp.sum(x * x, axis=1, keepdims=True)
        columns[0, pl.ds(i * 32, 32), :] = jnp.where(lane < 64, total, squares)
        acc[pl.ds(i * 32, 32), :] = x
        return carry

    lax.fori_loop(0, rows // 32, measure_rows, 0, unroll=UNROLL)
    turned = columns[0].T
    stats_out[0:8, :] = turned[0:8]
    stats_out[8:16, :] = turned[64:72]

    pl.semaphore_wait(barrier, LINE - 1 + IMAGES - 1)

    def stat_copy(r):
        return pltpu.make_async_remote_copy(
            src_ref=stats_out, dst_ref=stats_in.at[r - 1], send_sem=stat_send.at[r - 1],
            recv_sem=stat_recv.at[r - 1], device_id=(d, lax.rem(z + r, LINE)), device_id_type=MESH,
        )

    for r in range(1, LINE):
        stat_copy(r).start()
    for r in range(1, LINE):
        stat_copy(r).wait_recv()
    total = stats_out[...] + stats_in[0] + stats_in[1] + stats_in[2]
    mean = total[0:8] / width
    spread = total[8:16] / width - mean * mean
    scale = lax.rsqrt(spread + EPS)
    columns[0] = jnp.concatenate([mean] * (HEAD_DIM // 8), axis=0).T
    columns[1] = jnp.concatenate([scale] * (HEAD_DIM // 8), axis=0).T

    def normalize(i, carry):
        at = pl.ds(i * 32, 32)
        x = acc[at, :]
        scaled = (x - columns[0, at, 0:1]) * columns[1, at, 0:1]
        normed[0, at, :] = (scaled * gain[...][None, :]).astype(jnp.bfloat16)
        return carry

    lax.fori_loop(0, rows // 32, normalize, 0, unroll=UNROLL)

    piece = rows // PIECES

    def norm_copy(slot, to, offset, i):
        at = pl.ds(i * piece, piece)
        return pltpu.make_async_remote_copy(
            src_ref=normed.at[slot, at], dst_ref=normed.at[to, at], send_sem=norm_send.at[to],
            recv_sem=norm_recv.at[to, i], device_id=(d ^ offset, z), device_id_type=MESH,
        )

    near, far = image_of(1, core), image_of(2, core)
    for p in (near, 1):
        for i in range(PIECES):
            norm_copy(0, p, p, i).start()


    def ready(c, i):
        @pl.when((lax.rem(c, 2) == 1) & (c < CHUNKS - 1))
        def _():
            p = image_of((c + 1) // 2, core)
            norm_copy(0, p, p, i).wait_recv()

            @pl.when(lax.rem(p, 2) == 0)
            def _():
                norm_copy(p, p + 1, 1, i).start()

    def sum_copy(t, c, i):
        part = sums.at[t, c, i * piece : (i + 1) * piece]
        return pltpu.make_async_remote_copy(
            src_ref=part, dst_ref=part, send_sem=sum_send.at[t],
            recv_sem=sum_recv.at[t, lax.rem(c, TURNS), i], device_id=(d, lax.rem(z + 2 * t - 1 + LINE, LINE)),
            device_id_type=MESH,
        )

    def give_copy(t, c, i):
        part = given.at[t, c, i * piece : (i + 1) * piece]
        return pltpu.make_async_remote_copy(
            src_ref=part, dst_ref=part, send_sem=give_send.at[t],
            recv_sem=give_recv.at[t, lax.rem(c, TURNS), i], device_id=(d, lax.rem(z + 1 - 2 * t + LINE, LINE)),
            device_id_type=MESH,
        )

    def part_copy(p):
        return pltpu.make_async_remote_copy(
            src_ref=sent.at[p - 1], dst_ref=got.at[p - 1], send_sem=part_send.at[p - 1],
            recv_sem=part_recv.at[p - 1], device_id=(d ^ p, z), device_id_type=MESH,
        )

    def term(c, t, at):
        return jnp.dot(
            normed[image_of((c + 1) // 2, core), at, :], wv[2 * t + lax.rem(c + 1, 2)], preferred_element_type=jnp.float32
        )

    def prepare(k):
        def one(t, carry):
            s = position(t)
            c = k - s

            @pl.when((s > 0) & (c >= 0) & (c < CHUNKS))
            def _():
                @pl.when(s == 1)
                def _():
                    for i in range(PIECES):
                        ready(c, i)

                terms[t] = term(c, t, slice(None))

            return carry

        lax.fori_loop(0, 2, one, 0)

    for item in loads[1:]:
        item.wait()

    def head_unit(values):
        mean = jnp.mean(values, axis=-1, keepdims=True)
        centered = values - mean
        spread = jnp.mean(centered * centered, axis=-1, keepdims=True)
        return centered * lax.rsqrt(spread + EPS)

    def finish(t, c):
        def column(i):
            value = terms[t, :, i * HEAD_DIM : (i + 1) * HEAD_DIM]
            value = value + sums[t, c, :, i * HEAD_DIM : (i + 1) * HEAD_DIM].astype(jnp.float32)
            return value.astype(jnp.bfloat16)

        query = head_unit(column(0).astype(jnp.float32)) * (1.0 / HEAD_DIM) ** 0.5
        keys = head_unit(column(1).astype(jnp.float32)).astype(jnp.bfloat16)
        scores = lax.dot_general(
            query.astype(jnp.bfloat16), keys, (((1,), (1,)), ((), ())), preferred_element_type=jnp.float32
        )
        weights = jnp.exp(scores)
        probs = (weights / jnp.sum(weights, axis=-1, keepdims=True)).astype(jnp.bfloat16)
        mixed = jnp.dot(probs, column(2), preferred_element_type=jnp.float32)
        given[t, c, :, :HEAD_DIM] = mixed.astype(jnp.bfloat16)
        for i in range(up_block // HEAD_DIM):
            u = column(3 + i).astype(jnp.float32)
            given[t, c, :, (1 + i) * HEAD_DIM : (2 + i) * HEAD_DIM] = jax.nn.gelu(u).astype(jnp.bfloat16)

    def sent_from(whole, sem):
        pltpu.make_async_remote_copy(
            src_ref=whole, dst_ref=whole, send_sem=sem, recv_sem=sem,
            device_id=(d, lax.rem(z + 1, LINE)), device_id_type=MESH,
        ).wait_send()

    def step(k, carry):
        def stream(n):
            return jnp.where(z < LINE // 2, 1 - n, n)

        def move_sums(n, carry, i):
            t = stream(n)
            t = jnp.where((z > 0) & (z < LINE - 1), 1 - t, t)
            s = position(t)
            c = k - s

            @pl.when((c >= 0) & (c < CHUNKS))
            def _():
                at = pl.ds(i * piece, piece)

                @pl.when(s > 0)
                def _():
                    sum_copy(t, c, i).wait_recv()

                @pl.when(s == 0)
                def _():
                    ready(c, i)
                    sums[t, c, at, :] = term(c, t, at).astype(jnp.bfloat16)
                    sum_copy(t, c, i).start()

                @pl.when((s > 0) & (s < LINE - 1))
                def _():
                    value = terms[t, at, :] + sums[t, c, at, :].astype(jnp.float32)
                    sums[t, c, at, :] = value.astype(jnp.bfloat16)
                    sum_copy(t, c, i).start()

                if i == PIECES - 1:

                    @pl.when(s == LINE - 1)
                    def _():
                        finish(t, c)
                        for j in range(PIECES):
                            give_copy(t, c, j).start()

            return carry

        for i in range(PIECES):
            lax.fori_loop(0, 2, functools.partial(move_sums, i=i), 0)

        def move_given(n, carry):
            t = stream(n)
            s = position(t)
            c = k - 2 * (LINE - 1) + s

            @pl.when((c >= 0) & (c < CHUNKS) & (s < LINE - 1))
            def _():
                for i in range(PIECES):
                    give_copy(t, c, i).wait_recv()

                    @pl.when(s > 0)
                    def _():
                        give_copy(t, c, i).start()

            return carry

        lax.fori_loop(0, 2, move_given, 0)
        @pl.when(k == 1)
        def _():
            sent_from(normed.at[0], norm_send.at[near])
            for i in range(PIECES):
                norm_copy(0, far, far, i).start()

        @pl.when(k == 3)
        def _():
            for i in range(PIECES):
                norm_copy(0, 6, 6, i).start()

        prepare(k + 1)

        c = k - 2 * (LINE - 1) + jnp.minimum(z, LINE - 1 - z)

        def tiles(work):
            def one(n, carry):
                work(pl.ds(n * 256, 256))
                return carry

            lax.fori_loop(0, out_cols // 256, one, 0)

        def own(t, c):
            def one(at):
                acc[:, at] = acc[:, at] + jnp.dot(
                    given[t, c], wo[2 * t + lax.rem(c + 1, 2), :, at], preferred_element_type=jnp.float32
                )

            tiles(one)

        @pl.when((c == 0) | (c == CHUNKS - 1))
        def _():
            own(stream(0), c)

            @pl.when(c == 0)
            def _():
                own(stream(1), c)

        @pl.when(c == CHUNKS - 3 + jnp.minimum(z, LINE - 1 - z))
        def _():
            own(stream(1), CHUNKS - 1)

        @pl.when((c >= 2) & (c < CHUNKS) & (lax.rem(c, 2) == 0))
        def _():
            p = image_of(c // 2, core)

            def other(at):
                value = jnp.zeros((rows, 256), jnp.float32)
                for t in range(2):
                    for h, chunk in enumerate((c - 1, c)):
                        value = value + jnp.dot(
                            given[t, chunk], wo[2 * t + h, :, at], preferred_element_type=jnp.float32
                        )
                sent[p - 1, :, at] = value.astype(jnp.bfloat16)

            tiles(other)
            part_copy(p).start()

            @pl.when((c >= 4) & (c < CHUNKS - 2))
            def _():
                collect(c // 2 - 1)

        return carry

    def arrival(pair):
        p = pick(pair, ORDER)
        return image_of(pair, jnp.where(lax.rem(p, 2) == 1, 1 - core, core))

    def collect(pair):
        p = arrival(pair)
        part_copy(p).wait_recv()

        def add(i, carry):
            at = pl.ds(i * 32, 32)
            acc[at, :] = acc[at, :] + got[p - 1, at, :].astype(jnp.float32)
            return carry

        lax.fori_loop(0, rows // 32, add, 0)

    lax.fori_loop(0, CHUNKS + 2 * (LINE - 1), step, 0)

    last = arrival(CHUNKS // 2 - 2)
    part_copy(last).wait_recv()
    part_copy(1).wait_recv()

    def write(i, carry):
        at = pl.ds(i * 32, 32)
        value = acc[at, :] + got[last - 1, at, :].astype(jnp.float32)
        out[at, :] = (value + got[0, at, :].astype(jnp.float32)).astype(jnp.bfloat16)
        return carry

    lax.fori_loop(0, rows // 32, write, 0)

    for r in range(1, LINE):
        stat_copy(r).wait_send()
    for p in (1, far, 6):
        sent_from(normed.at[0], norm_send.at[p])
    for p in (2, 4, 6):
        sent_from(normed.at[p], norm_send.at[p + 1])

    for t in range(2):

        @pl.when(position(t) < LINE - 1)
        def _():
            sent_from(sums.at[t], sum_send.at[t])

        @pl.when(position(t) > 0)
        def _():
            sent_from(given.at[t], give_send.at[t])

    for p in range(1, IMAGES):
        part_copy(p).wait_send()


def on_line(tokens, norm_gain, w_qkv, w_up, w_attn_out, w_down):
    rows, feat = tokens.shape
    units = w_up.shape[1]
    up_block = units // BLOCKS
    out_cols = w_down.shape[1]
    cols = 3 * HEAD_DIM + up_block
    hidden = HEAD_DIM + up_block
    w_heads = w_qkv.transpose(1, 0, 2)
    anywhere = pl.BlockSpec(memory_space=pl.ANY)
    inside = pl.BlockSpec(memory_space=pltpu.VMEM)
    dma = pltpu.SemaphoreType.DMA
    return pl.pallas_call(
        line_kernel,
        out_shape=pltpu.VMEM((rows, out_cols), jnp.bfloat16),
        in_specs=[anywhere, inside] + [anywhere] * 4,
        out_specs=inside,
        scratch_shapes=[
            pltpu.VMEM((rows, feat), jnp.bfloat16),
            pltpu.VMEM((BLOCKS, feat, cols), jnp.bfloat16),
            pltpu.VMEM((BLOCKS, hidden, out_cols), jnp.bfloat16),
            pltpu.VMEM((IMAGES, rows, feat), jnp.bfloat16),
            pltpu.VMEM((2, CHUNKS, rows, cols), jnp.bfloat16),
            pltpu.VMEM((2, CHUNKS, rows, hidden), jnp.bfloat16),
            pltpu.VMEM((IMAGES - 1, rows, out_cols), jnp.bfloat16),
            pltpu.VMEM((IMAGES - 1, rows, out_cols), jnp.bfloat16),
            pltpu.VMEM((2, rows, cols), jnp.float32),
            pltpu.VMEM((rows, out_cols), jnp.float32),
            pltpu.VMEM((2, rows, HEAD_DIM), jnp.float32),
            pltpu.VMEM((16, rows), jnp.float32),
            pltpu.VMEM((LINE - 1, 16, rows), jnp.float32),
            dma((1 + 6 * BLOCKS,)),
            dma((LINE - 1,)),
            dma((LINE - 1,)),
            dma((IMAGES,)),
            dma((IMAGES, PIECES)),
            dma((2,)),
            dma((2, TURNS, PIECES)),
            dma((2,)),
            dma((2, TURNS, PIECES)),
            dma((IMAGES - 1,)),
            dma((IMAGES - 1,)),
        ],
        compiler_params=pltpu.CompilerParams(
            collective_id=0, has_side_effects=True, vmem_limit_bytes=66_000_000
        ),
    )(tokens, norm_gain, w_heads, w_up, w_attn_out, w_down)


def solution(mesh):
    placed = (
        P("dp", "mp"),
        P("mp"),
        P("mp", None, "dp"),
        P("mp", "dp"),
        P("dp", "mp"),
        P("dp", "mp"),
    )
    return jax.shard_map(
        local, mesh=mesh, in_specs=placed, out_specs=P("dp", "mp"), check_vma=False
    )
```

```python
import functools

import jax
import jax.numpy as jnp
from jax import lax
from jax.experimental import pallas as pl
from jax.experimental.pallas import tpu as pltpu
from jax.sharding import PartitionSpec as P

MESH = pl.DeviceIdType.MESH

HEAD_DIM = 128
PATCHES = 256


EPS = 1e-06
UP_SHARES = (1, 2, 2, 1)
FIRST = 1
LAG = 2


def normalize_rows(values, total, squares, gain, width):
    mean = total / width
    spread = squares / width - mean * mean
    scaled = (values - mean[:, None]) * lax.rsqrt(spread + EPS)[:, None]
    return (scaled * gain[None, :]).astype(jnp.bfloat16)


def head_norm(values):
    mean = jnp.mean(values, axis=-1, keepdims=True)
    centered = values - mean
    spread = jnp.mean(centered * centered, axis=-1, keepdims=True)
    return centered * lax.rsqrt(spread + EPS)


def attend(qkv, heads_here):
    rows = qkv.shape[0]
    images = rows // PATCHES
    parts = qkv.reshape(images, PATCHES, 3, heads_here, HEAD_DIM)
    query = (head_norm(parts[:, :, 0].astype(jnp.float32)) * (1.0 / HEAD_DIM) ** 0.5).astype(
        jnp.bfloat16
    )
    keys = head_norm(parts[:, :, 1].astype(jnp.float32)).astype(jnp.bfloat16)
    values = parts[:, :, 2]
    scores = jnp.einsum("iqhd,ikhd->ihqk", query, keys, preferred_element_type=jnp.float32)
    weights = jnp.exp(scores)
    probs = (weights / jnp.sum(weights, axis=-1, keepdims=True)).astype(jnp.bfloat16)
    mixed = jnp.einsum("ihqk,ikhd->iqhd", probs, values, preferred_element_type=jnp.float32)
    return mixed.astype(jnp.bfloat16).reshape(rows, heads_here * HEAD_DIM)


def shift(values, axis, senders, step):
    return lax.ppermute(values, axis, [(i, i + step) for i in senders])


def rows_of(values, block, count):
    return lax.dynamic_slice_in_dim(values, block * count, count, 0)


def add_rounded(*terms):
    total = terms[0].astype(jnp.float32)
    for term in terms[1:]:
        total = total + term.astype(jnp.float32)
    return total.astype(jnp.bfloat16)


class Group:
    def __init__(self, terms, finish, n, me, count):
        self.terms, self.finish, self.n, self.me, self.count = terms, finish, n, me, count
        self.right = self.left = self.own = None
        self.from_left, self.from_right = [], []

    def inputs(self, kind, step):
        n, me, count = self.n, self.me, self.count
        if kind == "scatter":
            send_right = rows_of(self.terms, (me - step - 1) % n, count)
            send_left = rows_of(self.terms, (me + step + 1) % n, count)
            if step:
                send_right = add_rounded(self.right, send_right)
                send_left = add_rounded(self.left, send_left)
            return send_right, send_left
        if step == 0:
            total = add_rounded(rows_of(self.terms, me, count), self.right, self.left)
            self.own = self.finish(total)
            return self.own, self.own
        return self.from_left[-1], self.from_right[-1]

    def move(self, kind, step, send_right, send_left):
        n = self.n
        if kind == "scatter":
            self.right = shift(send_right, "mp", range(step + 1), 1)
            self.left = shift(send_left, "mp", range(n - 1 - step, n), -1)
            return [self.right, self.left]
        self.from_left.append(shift(send_right, "mp", range(step, n - 1), 1))
        self.from_right.append(shift(send_left, "mp", range(1, n - step), -1))
        return [self.from_left[-1], self.from_right[-1]]

    def block(self, r):
        if r == 0:
            return self.own
        near, far = self.from_right[r - 1], self.from_left[self.n - r - 1]
        return jnp.where(self.me + r < self.n, near, far)


def run_line(groups, n):
    if n == 4:
        scatter_at, gather_at, period = [-3, -1, 0], [2, 5, 7], 4
    else:
        scatter_at, gather_at, period = [s - n + 2 for s in range(n - 1)], [2 + s for s in range(n - 1)], n
    slots = {}
    for g, group in enumerate(groups):
        for s in range(n - 1):
            slots.setdefault(g * period + gather_at[s], []).append((group, "gather", s))
            slots.setdefault(g * period + scatter_at[s], []).append((group, "scatter", s))
    history = []
    for at in sorted(slots):
        sends = [pair for group, kind, s in slots[at] for pair in group.inputs(kind, s)]
        if len(history) >= LAG:
            tied = lax.optimization_barrier(tuple(sends) + tuple(history[-LAG]))
            sends = tied[: len(sends)]
        moved = []
        for k, (group, kind, s) in enumerate(slots[at]):
            moved += group.move(kind, s, sends[2 * k], sends[2 * k + 1])
        history.append(moved)


def gather_normed(tokens, stats, n_dp, my_dp, normalize):
    rows, cols = tokens.shape
    if n_dp != 8:
        stats = lax.all_gather(stats, "dp", axis=1, tiled=True)
        return normalize(stats, lax.all_gather(tokens, "dp", axis=0, tiled=True), 0, n_dp)

    def hop(values, offset):
        return lax.ppermute(values, "dp", [(i, i ^ offset) for i in range(n_dp)])

    half = rows // 2
    held = {0: tokens, 2: hop(tokens, 2), 4: hop(tokens, 4)}
    held[1] = hop(tokens, 1)
    stats, held[2], held[4] = lax.optimization_barrier((stats, held[2], held[4]))
    stats = lax.all_gather(stats, "dp", axis=1, tiled=True)
    upper, lower = hop(held[2][:half], 4), hop(held[4][half:], 2)
    held[6] = jnp.concatenate([upper, lower])
    for offset in (2, 4, 6):
        held[offset ^ 1] = hop(held[offset], 1)
    result = jnp.zeros((n_dp * rows, cols), jnp.bfloat16)
    for offset in (0, 1, 2, 3, 4, 5, 6, 7):
        index = my_dp ^ offset
        result = lax.dynamic_update_slice_in_dim(
            result, normalize(stats, held[offset], index, 1), index * rows, 0
        )
    return result


def swap(values, bit, mine, dim, size):
    keep = lax.dynamic_index_in_dim(values, mine, dim, keepdims=False)
    give = lax.dynamic_index_in_dim(values, 1 - mine, dim, keepdims=False)
    got = lax.ppermute(give, "dp", [(i, i ^ (1 << bit)) for i in range(size)])
    return keep, got


def local(tokens, norm_gain, w_qkv, w_up, w_attn_out, w_down):
    if fits_line(tokens, w_qkv, w_up):
        return on_line(tokens, norm_gain, w_qkv, w_up, w_attn_out, w_down)
    n_mp, n_dp = lax.axis_size("mp"), lax.axis_size("dp")
    me, my_dp = lax.axis_index("mp"), lax.axis_index("dp")
    rows_here, feat_here = tokens.shape
    head_cols = w_qkv.shape[2]
    heads_here = head_cols // HEAD_DIM
    units = w_up.shape[1]
    width = feat_here * n_mp
    count = rows_here * n_dp // n_mp
    tokens_f = tokens.astype(jnp.float32)

    stats = lax.psum(
        jnp.stack([jnp.sum(tokens_f, axis=1), jnp.sum(tokens_f * tokens_f, axis=1)]), "mp"
    )

    def normalize(stats, block, index, many):
        here = lax.dynamic_slice_in_dim(stats, index * rows_here, many * rows_here, 1)
        return normalize_rows(block.astype(jnp.float32), here[0], here[1], norm_gain, width)

    normed = gather_normed(tokens, stats, n_dp, my_dp, normalize)

    halves = 2 if heads_here % 2 == 0 else 1
    group_heads = heads_here // halves
    group_cols = group_heads * HEAD_DIM

    def attention(projected):
        return attend(projected.reshape(count, 3, group_cols), group_heads)

    def activation(projected):
        return jax.nn.gelu(projected.astype(jnp.float32)).astype(jnp.bfloat16)

    heads = [("heads", g * group_cols, group_cols) for g in range(halves)]
    ups, first = [], 0
    for share in UP_SHARES:
        ups.append(("up", first, units * share // sum(UP_SHARES)))
        first += units * share // sum(UP_SHARES)
    groups = []
    weights_out = []
    for kind, start, size in ups[:FIRST] + heads + ups[FIRST:]:
        if kind == "heads":
            weight = w_qkv[:, :, start : start + size].reshape(feat_here, 3 * size)
            finish, weight_out = attention, w_attn_out[start : start + size]
        else:
            weight = w_up[:, start : start + size]
            finish, weight_out = activation, w_down[start : start + size]
        terms = jnp.dot(normed, weight, preferred_element_type=jnp.float32).astype(jnp.bfloat16)
        groups.append(Group(terms, finish, n_mp, me, count))
        weights_out.append(weight_out)
    run_line(groups, n_mp)

    order = sorted(range(n_mp), key=lambda r: min(r, n_mp - r))
    out_cols = w_down.shape[1]
    bits = n_dp.bit_length() - 1
    core = my_dp % 2
    pairs = count // rows_here // 2
    kept = jnp.zeros((n_mp * pairs, rows_here, out_cols), jnp.bfloat16)
    for r in order:
        block = sum(
            jnp.dot(group.block(r), weight, preferred_element_type=jnp.float32)
            for group, weight in zip(groups, weights_out)
        ).astype(jnp.bfloat16)
        block = block.reshape(pairs, 2, rows_here, out_cols)
        keep, got = swap(block, 0, core, 1, n_dp)
        kept = lax.dynamic_update_slice_in_dim(
            kept, add_rounded(keep, got), (me + r) % n_mp * pairs, 0
        )
    rest = list(range(1, bits))
    half = out_cols // 2
    results = []
    for part, bit_order in enumerate((rest, rest[::-1])):
        values = kept[:, :, part * half : (part + 1) * half].reshape(
            [2] * len(rest) + [rows_here, half]
        )
        left_bits = list(rest)
        base = tokens_f[:, part * half : (part + 1) * half]
        for bit in bit_order:
            dim = len(left_bits) - 1 - left_bits.index(bit)
            keep, got = swap(values, bit, (my_dp >> bit) % 2, dim, n_dp)
            left_bits.remove(bit)
            if left_bits:
                values = add_rounded(keep, got)
            else:
                total = base + (keep.astype(jnp.float32) + got.astype(jnp.float32))
                results.append(total.astype(jnp.bfloat16))
    return jnp.concatenate(results, axis=1)


BLOCKS = 4
IMAGES = 8
CHUNKS = 2 * IMAGES
LINE = 4
PIECES = 2
TURNS = 8
UNROLL = 4
ORDER = (0, 2, 4, 6, 7, 3, 5, 1, 0)


def fits_line(tokens, w_qkv, w_up):
    return (
        lax.axis_size("mp") == LINE
        and lax.axis_size("dp") == IMAGES
        and tokens.shape[0] == PATCHES
        and w_qkv.shape[2] == BLOCKS * HEAD_DIM
        and w_up.shape[1] % (BLOCKS * HEAD_DIM) == 0
    )


def pick(index, table):
    value = table[-1]
    for i in range(len(table) - 2, -1, -1):
        value = jnp.where(index == i, table[i], value)
    return value


def image_of(pair, core):
    offset = pick(pair, ORDER)
    crossed = pick(offset, (0, 1, 4, 5, 2, 3, 6, 7))
    return jnp.where(core == 1, crossed, offset)


def line_kernel(
    tokens, gain, w_heads, w_up, w_attn_out, w_down, out,
    tok, wv, wo, normed, sums, given, sent, got, terms, acc,
    columns, stats_out, stats_in,
    load_sem, stat_send, stat_recv, norm_send, norm_recv,
    sum_send, sum_recv, give_send, give_recv, part_send, part_recv,
):
    d, z = lax.axis_index("dp"), lax.axis_index("mp")
    core = lax.rem(d, 2)
    rows, feat = tok.shape
    width = feat * LINE
    up_block = w_up.shape[1] // BLOCKS
    out_cols = out.shape[1]
    hidden = HEAD_DIM + up_block

    def position(t):
        return jnp.where(t == 1, z, LINE - 1 - z)

    def load(src, dst, k):
        return pltpu.make_async_copy(src, dst, load_sem.at[k])

    loads = [load(tokens, tok, 0)]
    for j in range(BLOCKS):
        for i in range(3):
            loads.append(
                load(
                    w_heads.at[i, :, j * HEAD_DIM : (j + 1) * HEAD_DIM],
                    wv.at[j, :, i * HEAD_DIM : (i + 1) * HEAD_DIM],
                    1 + 6 * j + i,
                )
            )
        loads.append(
            load(w_up.at[:, j * up_block : (j + 1) * up_block], wv.at[j, :, 3 * HEAD_DIM :], 4 + 6 * j)
        )
    for j in range(BLOCKS):
        loads.append(
            load(w_attn_out.at[j * HEAD_DIM : (j + 1) * HEAD_DIM], wo.at[j, :HEAD_DIM], 5 + 6 * j)
        )
        loads.append(load(w_down.at[j * up_block : (j + 1) * up_block], wo.at[j, HEAD_DIM:], 6 + 6 * j))
    barrier = pltpu.get_barrier_semaphore()
    for r in range(1, LINE):
        pl.semaphore_signal(barrier, inc=1, device_id=(d, lax.rem(z + r, LINE)), device_id_type=MESH)
    loads[0].start()
    for p in range(1, IMAGES):
        pl.semaphore_signal(barrier, inc=1, device_id=(d ^ p, z), device_id_type=MESH)
    for item in loads[1:]:
        item.start()

    loads[0].wait()
    lane = lax.broadcasted_iota(jnp.int32, (32, HEAD_DIM), 1)

    def measure_rows(i, carry):
        x = tok[pl.ds(i * 32, 32), :].astype(jnp.float32)
        total = jnp.sum(x, axis=1, keepdims=True)
        squares = jnp.sum(x * x, axis=1, keepdims=True)
        columns[0, pl.ds(i * 32, 32), :] = jnp.where(lane < 64, total, squares)
        acc[pl.ds(i * 32, 32), :] = x
        return carry

    lax.fori_loop(0, rows // 32, measure_rows, 0, unroll=UNROLL)
    turned = columns[0].T
    stats_out[0:8, :] = turned[0:8]
    stats_out[8:16, :] = turned[64:72]

    pl.semaphore_wait(barrier, LINE - 1 + IMAGES - 1)

    def stat_copy(r):
        return pltpu.make_async_remote_copy(
            src_ref=stats_out, dst_ref=stats_in.at[r - 1], send_sem=stat_send.at[r - 1],
            recv_sem=stat_recv.at[r - 1], device_id=(d, lax.rem(z + r, LINE)), device_id_type=MESH,
        )

    for r in range(1, LINE):
        stat_copy(r).start()
    for r in range(1, LINE):
        stat_copy(r).wait_recv()
    total = stats_out[...] + stats_in[0] + stats_in[1] + stats_in[2]
    mean = total[0:8] / width
    spread = total[8:16] / width - mean * mean
    scale = lax.rsqrt(spread + EPS)
    columns[0] = jnp.concatenate([mean] * (HEAD_DIM // 8), axis=0).T
    columns[1] = jnp.concatenate([scale] * (HEAD_DIM // 8), axis=0).T

    def normalize(i, carry):
        at = pl.ds(i * 32, 32)
        x = acc[at, :]
        scaled = (x - columns[0, at, 0:1]) * columns[1, at, 0:1]
        normed[0, at, :] = (scaled * gain[...][None, :]).astype(jnp.bfloat16)
        return carry

    lax.fori_loop(0, rows // 32, normalize, 0, unroll=UNROLL)

    piece = rows // PIECES

    def norm_copy(slot, to, offset, i):
        at = pl.ds(i * piece, piece)
        return pltpu.make_async_remote_copy(
            src_ref=normed.at[slot, at], dst_ref=normed.at[to, at], send_sem=norm_send.at[to],
            recv_sem=norm_recv.at[to, i], device_id=(d ^ offset, z), device_id_type=MESH,
        )

    near, far = image_of(1, core), image_of(2, core)
    for p in (near, 1):
        for i in range(PIECES):
            norm_copy(0, p, p, i).start()


    def ready(c, i):
        @pl.when((lax.rem(c, 2) == 1) & (c < CHUNKS - 1))
        def _():
            p = image_of((c + 1) // 2, core)
            norm_copy(0, p, p, i).wait_recv()

            @pl.when(lax.rem(p, 2) == 0)
            def _():
                norm_copy(p, p + 1, 1, i).start()

    def sum_copy(t, c, i):
        part = sums.at[t, c, i * piece : (i + 1) * piece]
        return pltpu.make_async_remote_copy(
            src_ref=part, dst_ref=part, send_sem=sum_send.at[t],
            recv_sem=sum_recv.at[t, lax.rem(c, TURNS), i], device_id=(d, lax.rem(z + 2 * t - 1 + LINE, LINE)),
            device_id_type=MESH,
        )

    def give_copy(t, c, i):
        part = given.at[t, c, i * piece : (i + 1) * piece]
        return pltpu.make_async_remote_copy(
            src_ref=part, dst_ref=part, send_sem=give_send.at[t],
            recv_sem=give_recv.at[t, lax.rem(c, TURNS), i], device_id=(d, lax.rem(z + 1 - 2 * t + LINE, LINE)),
            device_id_type=MESH,
        )

    def part_copy(p):
        return pltpu.make_async_remote_copy(
            src_ref=sent.at[p - 1], dst_ref=got.at[p - 1], send_sem=part_send.at[p - 1],
            recv_sem=part_recv.at[p - 1], device_id=(d ^ p, z), device_id_type=MESH,
        )

    def term(c, t, at):
        return jnp.dot(
            normed[image_of((c + 1) // 2, core), at, :], wv[2 * t + lax.rem(c + 1, 2)], preferred_element_type=jnp.float32
        )

    def prepare(k):
        def one(t, carry):
            s = position(t)
            c = k - s

            @pl.when((s > 0) & (c >= 0) & (c < CHUNKS))
            def _():
                @pl.when(s == 1)
                def _():
                    for i in range(PIECES):
                        ready(c, i)

                terms[t] = term(c, t, slice(None))

            return carry

        lax.fori_loop(0, 2, one, 0)

    for item in loads[1:]:
        item.wait()

    def head_unit(values):
        mean = jnp.mean(values, axis=-1, keepdims=True)
        centered = values - mean
        spread = jnp.mean(centered * centered, axis=-1, keepdims=True)
        return centered * lax.rsqrt(spread + EPS)

    def finish(t, c):
        def column(i):
            value = terms[t, :, i * HEAD_DIM : (i + 1) * HEAD_DIM]
            value = value + sums[t, c, :, i * HEAD_DIM : (i + 1) * HEAD_DIM].astype(jnp.float32)
            return value.astype(jnp.bfloat16)

        query = head_unit(column(0).astype(jnp.float32)) * (1.0 / HEAD_DIM) ** 0.5
        keys = head_unit(column(1).astype(jnp.float32)).astype(jnp.bfloat16)
        scores = lax.dot_general(
            query.astype(jnp.bfloat16), keys, (((1,), (1,)), ((), ())), preferred_element_type=jnp.float32
        )
        weights = jnp.exp(scores)
        probs = (weights / jnp.sum(weights, axis=-1, keepdims=True)).astype(jnp.bfloat16)
        mixed = jnp.dot(probs, column(2), preferred_element_type=jnp.float32)
        given[t, c, :, :HEAD_DIM] = mixed.astype(jnp.bfloat16)
        for i in range(up_block // HEAD_DIM):
            u = column(3 + i).astype(jnp.float32)
            given[t, c, :, (1 + i) * HEAD_DIM : (2 + i) * HEAD_DIM] = jax.nn.gelu(u).astype(jnp.bfloat16)

    def sent_from(whole, sem):
        pltpu.make_async_remote_copy(
            src_ref=whole, dst_ref=whole, send_sem=sem, recv_sem=sem,
            device_id=(d, lax.rem(z + 1, LINE)), device_id_type=MESH,
        ).wait_send()

    inner = (z > 0) & (z < LINE - 1)

    def step(k, carry):
        def stream(n):
            far = jnp.where(z < LINE // 2, 1 - n, n)
            return jnp.where(inner, 1 - far, far)

        def move_sums(t, i):
            s = position(t)
            c = k - s

            @pl.when((c >= 0) & (c < CHUNKS))
            def _():
                at = pl.ds(i * piece, piece)

                @pl.when(s > 0)
                def _():
                    sum_copy(t, c, i).wait_recv()

                @pl.when(s == 0)
                def _():
                    ready(c, i)
                    sums[t, c, at, :] = term(c, t, at).astype(jnp.bfloat16)
                    sum_copy(t, c, i).start()

                @pl.when((s > 0) & (s < LINE - 1))
                def _():
                    value = terms[t, at, :] + sums[t, c, at, :].astype(jnp.float32)
                    sums[t, c, at, :] = value.astype(jnp.bfloat16)
                    sum_copy(t, c, i).start()

                if i == PIECES - 1:

                    @pl.when(s == LINE - 1)
                    def _():
                        finish(t, c)
                        for j in range(PIECES):
                            give_copy(t, c, j).start()

        def move_given(t, c):
            @pl.when((c >= 0) & (c < CHUNKS))
            def _():
                for i in range(PIECES):
                    give_copy(t, c, i).wait_recv()
                    give_copy(t, c, i).start()

        def serve(n, carry):
            t = stream(n)
            for i in range(PIECES):
                move_sums(t, i)

            @pl.when(n == 1)
            def _():
                prepare(k + 1)

            c = k - 2 * (LINE - 1) + 1

            @pl.when(inner & ((n == 1) | (k <= CHUNKS + 2)))
            def _():
                move_given(t, c)

            @pl.when(inner & (n == 0) & (k >= CHUNKS + 2))
            def _():
                move_given(t, c + 1)

            return carry

        lax.fori_loop(0, 2, serve, 0)

        @pl.when(k == 1)
        def _():
            sent_from(normed.at[0], norm_send.at[near])
            for i in range(PIECES):
                norm_copy(0, far, far, i).start()

        @pl.when(k == 3)
        def _():
            for i in range(PIECES):
                norm_copy(0, 6, 6, i).start()

        @pl.when(jnp.logical_not(inner) & (k >= 2 * (LINE - 1)))
        def _():
            for i in range(PIECES):
                give_copy(stream(0), k - 2 * (LINE - 1), i).wait_recv()

        c = k - 2 * (LINE - 1) + jnp.minimum(z, LINE - 1 - z)

        def tiles(work):
            def one(n, carry):
                work(pl.ds(n * 256, 256))
                return carry

            lax.fori_loop(0, out_cols // 256, one, 0)

        def own(t, c):
            def one(at):
                acc[:, at] = acc[:, at] + jnp.dot(
                    given[t, c], wo[2 * t + lax.rem(c + 1, 2), :, at], preferred_element_type=jnp.float32
                )

            tiles(one)

        @pl.when((c == 0) | (c == CHUNKS - 1))
        def _():
            own(stream(0), c)

            @pl.when((c == 0) | inner)
            def _():
                own(stream(1), c)

        @pl.when((c == CHUNKS - 3) & jnp.logical_not(inner))
        def _():
            own(stream(1), CHUNKS - 1)

        @pl.when((c >= 2) & (c < CHUNKS) & (lax.rem(c, 2) == 0))
        def _():
            p = image_of(c // 2, core)

            def other(at):
                value = jnp.zeros((rows, 256), jnp.float32)
                for t in range(2):
                    for h, chunk in enumerate((c - 1, c)):
                        value = value + jnp.dot(
                            given[t, chunk], wo[2 * t + h, :, at], preferred_element_type=jnp.float32
                        )
                sent[p - 1, :, at] = value.astype(jnp.bfloat16)

            tiles(other)
            part_copy(p).start()

            @pl.when((c >= 4) & (c < CHUNKS - 2))
            def _():
                collect(c // 2 - 1)

        return carry

    def arrival(pair):
        p = pick(pair, ORDER)
        return image_of(pair, jnp.where(lax.rem(p, 2) == 1, 1 - core, core))

    def collect(pair):
        p = arrival(pair)
        part_copy(p).wait_recv()

        def add(i, carry):
            at = pl.ds(i * 32, 32)
            acc[at, :] = acc[at, :] + got[p - 1, at, :].astype(jnp.float32)
            return carry

        lax.fori_loop(0, rows // 32, add, 0)

    lax.fori_loop(0, CHUNKS + 2 * (LINE - 1), step, 0)

    last = arrival(CHUNKS // 2 - 2)
    part_copy(last).wait_recv()
    part_copy(1).wait_recv()

    def write(i, carry):
        at = pl.ds(i * 32, 32)
        value = acc[at, :] + got[last - 1, at, :].astype(jnp.float32)
        out[at, :] = (value + got[0, at, :].astype(jnp.float32)).astype(jnp.bfloat16)
        return carry

    lax.fori_loop(0, rows // 32, write, 0)

    for r in range(1, LINE):
        stat_copy(r).wait_send()
    for p in (1, far, 6):
        sent_from(normed.at[0], norm_send.at[p])
    for p in (2, 4, 6):
        sent_from(normed.at[p], norm_send.at[p + 1])

    for t in range(2):

        @pl.when(position(t) < LINE - 1)
        def _():
            sent_from(sums.at[t], sum_send.at[t])

        @pl.when(position(t) > 0)
        def _():
            sent_from(given.at[t], give_send.at[t])

    for p in range(1, IMAGES):
        part_copy(p).wait_send()


def on_line(tokens, norm_gain, w_qkv, w_up, w_attn_out, w_down):
    rows, feat = tokens.shape
    units = w_up.shape[1]
    up_block = units // BLOCKS
    out_cols = w_down.shape[1]
    cols = 3 * HEAD_DIM + up_block
    hidden = HEAD_DIM + up_block
    w_heads = w_qkv.transpose(1, 0, 2)
    anywhere = pl.BlockSpec(memory_space=pl.ANY)
    inside = pl.BlockSpec(memory_space=pltpu.VMEM)
    dma = pltpu.SemaphoreType.DMA
    return pl.pallas_call(
        line_kernel,
        out_shape=pltpu.VMEM((rows, out_cols), jnp.bfloat16),
        in_specs=[anywhere, inside] + [anywhere] * 4,
        out_specs=inside,
        scratch_shapes=[
            pltpu.VMEM((rows, feat), jnp.bfloat16),
            pltpu.VMEM((BLOCKS, feat, cols), jnp.bfloat16),
            pltpu.VMEM((BLOCKS, hidden, out_cols), jnp.bfloat16),
            pltpu.VMEM((IMAGES, rows, feat), jnp.bfloat16),
            pltpu.VMEM((2, CHUNKS, rows, cols), jnp.bfloat16),
            pltpu.VMEM((2, CHUNKS, rows, hidden), jnp.bfloat16),
            pltpu.VMEM((IMAGES - 1, rows, out_cols), jnp.bfloat16),
            pltpu.VMEM((IMAGES - 1, rows, out_cols), jnp.bfloat16),
            pltpu.VMEM((2, rows, cols), jnp.float32),
            pltpu.VMEM((rows, out_cols), jnp.float32),
            pltpu.VMEM((2, rows, HEAD_DIM), jnp.float32),
            pltpu.VMEM((16, rows), jnp.float32),
            pltpu.VMEM((LINE - 1, 16, rows), jnp.float32),
            dma((1 + 6 * BLOCKS,)),
            dma((LINE - 1,)),
            dma((LINE - 1,)),
            dma((IMAGES,)),
            dma((IMAGES, PIECES)),
            dma((2,)),
            dma((2, TURNS, PIECES)),
            dma((2,)),
            dma((2, TURNS, PIECES)),
            dma((IMAGES - 1,)),
            dma((IMAGES - 1,)),
        ],
        compiler_params=pltpu.CompilerParams(
            collective_id=0, has_side_effects=True, vmem_limit_bytes=66_000_000
        ),
    )(tokens, norm_gain, w_heads, w_up, w_attn_out, w_down)


def solution(mesh):
    placed = (
        P("dp", "mp"),
        P("mp"),
        P("mp", None, "dp"),
        P("mp", "dp"),
        P("dp", "mp"),
        P("dp", "mp"),
    )
    return jax.shard_map(
        local, mesh=mesh, in_specs=placed, out_specs=P("dp", "mp"), check_vma=False
    )
```

```python
import functools

import jax
import jax.numpy as jnp
from jax import lax
from jax.experimental import pallas as pl
from jax.experimental.pallas import tpu as pltpu
from jax.sharding import PartitionSpec as P

MESH = pl.DeviceIdType.MESH

HEAD_DIM = 128
PATCHES = 256


EPS = 1e-06
UP_SHARES = (1, 2, 2, 1)
FIRST = 1
LAG = 2


def normalize_rows(values, total, squares, gain, width):
    mean = total / width
    spread = squares / width - mean * mean
    scaled = (values - mean[:, None]) * lax.rsqrt(spread + EPS)[:, None]
    return (scaled * gain[None, :]).astype(jnp.bfloat16)


def head_norm(values):
    mean = jnp.mean(values, axis=-1, keepdims=True)
    centered = values - mean
    spread = jnp.mean(centered * centered, axis=-1, keepdims=True)
    return centered * lax.rsqrt(spread + EPS)


def attend(qkv, heads_here):
    rows = qkv.shape[0]
    images = rows // PATCHES
    parts = qkv.reshape(images, PATCHES, 3, heads_here, HEAD_DIM)
    query = (head_norm(parts[:, :, 0].astype(jnp.float32)) * (1.0 / HEAD_DIM) ** 0.5).astype(
        jnp.bfloat16
    )
    keys = head_norm(parts[:, :, 1].astype(jnp.float32)).astype(jnp.bfloat16)
    values = parts[:, :, 2]
    scores = jnp.einsum("iqhd,ikhd->ihqk", query, keys, preferred_element_type=jnp.float32)
    weights = jnp.exp(scores)
    probs = (weights / jnp.sum(weights, axis=-1, keepdims=True)).astype(jnp.bfloat16)
    mixed = jnp.einsum("ihqk,ikhd->iqhd", probs, values, preferred_element_type=jnp.float32)
    return mixed.astype(jnp.bfloat16).reshape(rows, heads_here * HEAD_DIM)


def shift(values, axis, senders, step):
    return lax.ppermute(values, axis, [(i, i + step) for i in senders])


def rows_of(values, block, count):
    return lax.dynamic_slice_in_dim(values, block * count, count, 0)


def add_rounded(*terms):
    total = terms[0].astype(jnp.float32)
    for term in terms[1:]:
        total = total + term.astype(jnp.float32)
    return total.astype(jnp.bfloat16)


class Group:
    def __init__(self, terms, finish, n, me, count):
        self.terms, self.finish, self.n, self.me, self.count = terms, finish, n, me, count
        self.right = self.left = self.own = None
        self.from_left, self.from_right = [], []

    def inputs(self, kind, step):
        n, me, count = self.n, self.me, self.count
        if kind == "scatter":
            send_right = rows_of(self.terms, (me - step - 1) % n, count)
            send_left = rows_of(self.terms, (me + step + 1) % n, count)
            if step:
                send_right = add_rounded(self.right, send_right)
                send_left = add_rounded(self.left, send_left)
            return send_right, send_left
        if step == 0:
            total = add_rounded(rows_of(self.terms, me, count), self.right, self.left)
            self.own = self.finish(total)
            return self.own, self.own
        return self.from_left[-1], self.from_right[-1]

    def move(self, kind, step, send_right, send_left):
        n = self.n
        if kind == "scatter":
            self.right = shift(send_right, "mp", range(step + 1), 1)
            self.left = shift(send_left, "mp", range(n - 1 - step, n), -1)
            return [self.right, self.left]
        self.from_left.append(shift(send_right, "mp", range(step, n - 1), 1))
        self.from_right.append(shift(send_left, "mp", range(1, n - step), -1))
        return [self.from_left[-1], self.from_right[-1]]

    def block(self, r):
        if r == 0:
            return self.own
        near, far = self.from_right[r - 1], self.from_left[self.n - r - 1]
        return jnp.where(self.me + r < self.n, near, far)


def run_line(groups, n):
    if n == 4:
        scatter_at, gather_at, period = [-3, -1, 0], [2, 5, 7], 4
    else:
        scatter_at, gather_at, period = [s - n + 2 for s in range(n - 1)], [2 + s for s in range(n - 1)], n
    slots = {}
    for g, group in enumerate(groups):
        for s in range(n - 1):
            slots.setdefault(g * period + gather_at[s], []).append((group, "gather", s))
            slots.setdefault(g * period + scatter_at[s], []).append((group, "scatter", s))
    history = []
    for at in sorted(slots):
        sends = [pair for group, kind, s in slots[at] for pair in group.inputs(kind, s)]
        if len(history) >= LAG:
            tied = lax.optimization_barrier(tuple(sends) + tuple(history[-LAG]))
            sends = tied[: len(sends)]
        moved = []
        for k, (group, kind, s) in enumerate(slots[at]):
            moved += group.move(kind, s, sends[2 * k], sends[2 * k + 1])
        history.append(moved)


def gather_normed(tokens, stats, n_dp, my_dp, normalize):
    rows, cols = tokens.shape
    if n_dp != 8:
        stats = lax.all_gather(stats, "dp", axis=1, tiled=True)
        return normalize(stats, lax.all_gather(tokens, "dp", axis=0, tiled=True), 0, n_dp)

    def hop(values, offset):
        return lax.ppermute(values, "dp", [(i, i ^ offset) for i in range(n_dp)])

    half = rows // 2
    held = {0: tokens, 2: hop(tokens, 2), 4: hop(tokens, 4)}
    held[1] = hop(tokens, 1)
    stats, held[2], held[4] = lax.optimization_barrier((stats, held[2], held[4]))
    stats = lax.all_gather(stats, "dp", axis=1, tiled=True)
    upper, lower = hop(held[2][:half], 4), hop(held[4][half:], 2)
    held[6] = jnp.concatenate([upper, lower])
    for offset in (2, 4, 6):
        held[offset ^ 1] = hop(held[offset], 1)
    result = jnp.zeros((n_dp * rows, cols), jnp.bfloat16)
    for offset in (0, 1, 2, 3, 4, 5, 6, 7):
        index = my_dp ^ offset
        result = lax.dynamic_update_slice_in_dim(
            result, normalize(stats, held[offset], index, 1), index * rows, 0
        )
    return result


def swap(values, bit, mine, dim, size):
    keep = lax.dynamic_index_in_dim(values, mine, dim, keepdims=False)
    give = lax.dynamic_index_in_dim(values, 1 - mine, dim, keepdims=False)
    got = lax.ppermute(give, "dp", [(i, i ^ (1 << bit)) for i in range(size)])
    return keep, got


def local(tokens, norm_gain, w_qkv, w_up, w_attn_out, w_down):
    if fits_line(tokens, w_qkv, w_up):
        return on_line(tokens, norm_gain, w_qkv, w_up, w_attn_out, w_down)
    n_mp, n_dp = lax.axis_size("mp"), lax.axis_size("dp")
    me, my_dp = lax.axis_index("mp"), lax.axis_index("dp")
    rows_here, feat_here = tokens.shape
    head_cols = w_qkv.shape[2]
    heads_here = head_cols // HEAD_DIM
    units = w_up.shape[1]
    width = feat_here * n_mp
    count = rows_here * n_dp // n_mp
    tokens_f = tokens.astype(jnp.float32)

    stats = lax.psum(
        jnp.stack([jnp.sum(tokens_f, axis=1), jnp.sum(tokens_f * tokens_f, axis=1)]), "mp"
    )

    def normalize(stats, block, index, many):
        here = lax.dynamic_slice_in_dim(stats, index * rows_here, many * rows_here, 1)
        return normalize_rows(block.astype(jnp.float32), here[0], here[1], norm_gain, width)

    normed = gather_normed(tokens, stats, n_dp, my_dp, normalize)

    halves = 2 if heads_here % 2 == 0 else 1
    group_heads = heads_here // halves
    group_cols = group_heads * HEAD_DIM

    def attention(projected):
        return attend(projected.reshape(count, 3, group_cols), group_heads)

    def activation(projected):
        return jax.nn.gelu(projected.astype(jnp.float32)).astype(jnp.bfloat16)

    heads = [("heads", g * group_cols, group_cols) for g in range(halves)]
    ups, first = [], 0
    for share in UP_SHARES:
        ups.append(("up", first, units * share // sum(UP_SHARES)))
        first += units * share // sum(UP_SHARES)
    groups = []
    weights_out = []
    for kind, start, size in ups[:FIRST] + heads + ups[FIRST:]:
        if kind == "heads":
            weight = w_qkv[:, :, start : start + size].reshape(feat_here, 3 * size)
            finish, weight_out = attention, w_attn_out[start : start + size]
        else:
            weight = w_up[:, start : start + size]
            finish, weight_out = activation, w_down[start : start + size]
        terms = jnp.dot(normed, weight, preferred_element_type=jnp.float32).astype(jnp.bfloat16)
        groups.append(Group(terms, finish, n_mp, me, count))
        weights_out.append(weight_out)
    run_line(groups, n_mp)

    order = sorted(range(n_mp), key=lambda r: min(r, n_mp - r))
    out_cols = w_down.shape[1]
    bits = n_dp.bit_length() - 1
    core = my_dp % 2
    pairs = count // rows_here // 2
    kept = jnp.zeros((n_mp * pairs, rows_here, out_cols), jnp.bfloat16)
    for r in order:
        block = sum(
            jnp.dot(group.block(r), weight, preferred_element_type=jnp.float32)
            for group, weight in zip(groups, weights_out)
        ).astype(jnp.bfloat16)
        block = block.reshape(pairs, 2, rows_here, out_cols)
        keep, got = swap(block, 0, core, 1, n_dp)
        kept = lax.dynamic_update_slice_in_dim(
            kept, add_rounded(keep, got), (me + r) % n_mp * pairs, 0
        )
    rest = list(range(1, bits))
    half = out_cols // 2
    results = []
    for part, bit_order in enumerate((rest, rest[::-1])):
        values = kept[:, :, part * half : (part + 1) * half].reshape(
            [2] * len(rest) + [rows_here, half]
        )
        left_bits = list(rest)
        base = tokens_f[:, part * half : (part + 1) * half]
        for bit in bit_order:
            dim = len(left_bits) - 1 - left_bits.index(bit)
            keep, got = swap(values, bit, (my_dp >> bit) % 2, dim, n_dp)
            left_bits.remove(bit)
            if left_bits:
                values = add_rounded(keep, got)
            else:
                total = base + (keep.astype(jnp.float32) + got.astype(jnp.float32))
                results.append(total.astype(jnp.bfloat16))
    return jnp.concatenate(results, axis=1)


BLOCKS = 4
IMAGES = 8
CHUNKS = 2 * IMAGES
LINE = 4
PIECES = 2
TURNS = 6
UNROLL = 8
ORDER = (0, 2, 4, 6, 7, 3, 5, 1, 0)


def fits_line(tokens, w_qkv, w_up):
    return (
        lax.axis_size("mp") == LINE
        and lax.axis_size("dp") == IMAGES
        and tokens.shape[0] == PATCHES
        and w_qkv.shape[2] == BLOCKS * HEAD_DIM
        and w_up.shape[1] % (BLOCKS * HEAD_DIM) == 0
    )


def pick(index, table):
    value = table[-1]
    for i in range(len(table) - 2, -1, -1):
        value = jnp.where(index == i, table[i], value)
    return value


def image_of(pair, core):
    offset = pick(pair, ORDER)
    crossed = pick(offset, (0, 1, 4, 5, 2, 3, 6, 7))
    return jnp.where(core == 1, crossed, offset)


def line_kernel(
    tokens, gain, w_heads, w_up, w_attn_out, w_down, out,
    tok, wv, wo, normed, sums, given, sent, got, terms, acc,
    columns, stats_out, stats_in,
    load_sem, stat_send, stat_recv, norm_send, norm_recv,
    sum_send, sum_recv, give_send, give_recv, part_send, part_recv,
):
    d, z = lax.axis_index("dp"), lax.axis_index("mp")
    core = lax.rem(d, 2)
    rows, feat = tok.shape
    width = feat * LINE
    up_block = w_up.shape[1] // BLOCKS
    out_cols = out.shape[1]
    hidden = HEAD_DIM + up_block

    def position(t):
        return jnp.where(t == 1, z, LINE - 1 - z)

    def load(src, dst, k):
        return pltpu.make_async_copy(src, dst, load_sem.at[k])

    loads = [load(tokens, tok, 0)]
    for j in range(BLOCKS):
        for i in range(3):
            loads.append(
                load(
                    w_heads.at[i, :, j * HEAD_DIM : (j + 1) * HEAD_DIM],
                    wv.at[j, :, i * HEAD_DIM : (i + 1) * HEAD_DIM],
                    1 + 6 * j + i,
                )
            )
        loads.append(
            load(w_up.at[:, j * up_block : (j + 1) * up_block], wv.at[j, :, 3 * HEAD_DIM :], 4 + 6 * j)
        )
    for j in range(BLOCKS):
        loads.append(
            load(w_attn_out.at[j * HEAD_DIM : (j + 1) * HEAD_DIM], wo.at[j, :HEAD_DIM], 5 + 6 * j)
        )
        loads.append(load(w_down.at[j * up_block : (j + 1) * up_block], wo.at[j, HEAD_DIM:], 6 + 6 * j))
    barrier = pltpu.get_barrier_semaphore()
    for r in range(1, LINE):
        pl.semaphore_signal(barrier, inc=1, device_id=(d, lax.rem(z + r, LINE)), device_id_type=MESH)
    loads[0].start()
    for p in range(1, IMAGES):
        pl.semaphore_signal(barrier, inc=1, device_id=(d ^ p, z), device_id_type=MESH)
    for item in loads[1:]:
        item.start()

    loads[0].wait()
    lane = lax.broadcasted_iota(jnp.int32, (32, HEAD_DIM), 1)

    def measure_rows(i, carry):
        x = tok[pl.ds(i * 32, 32), :].astype(jnp.float32)
        total = jnp.sum(x, axis=1, keepdims=True)
        squares = jnp.sum(x * x, axis=1, keepdims=True)
        columns[0, pl.ds(i * 32, 32), :] = jnp.where(lane < 64, total, squares)
        acc[pl.ds(i * 32, 32), :] = x
        return carry

    lax.fori_loop(0, rows // 32, measure_rows, 0, unroll=UNROLL)
    turned = columns[0].T
    stats_out[0:8, :] = turned[0:8]
    stats_out[8:16, :] = turned[64:72]

    pl.semaphore_wait(barrier, LINE - 1 + IMAGES - 1)

    def stat_copy(r):
        return pltpu.make_async_remote_copy(
            src_ref=stats_out, dst_ref=stats_in.at[r - 1], send_sem=stat_send.at[r - 1],
            recv_sem=stat_recv.at[r - 1], device_id=(d, lax.rem(z + r, LINE)), device_id_type=MESH,
        )

    for r in range(1, LINE):
        stat_copy(r).start()
    for r in range(1, LINE):
        stat_copy(r).wait_recv()
    total = stats_out[...] + stats_in[0] + stats_in[1] + stats_in[2]
    mean = total[0:8] / width
    spread = total[8:16] / width - mean * mean
    scale = lax.rsqrt(spread + EPS)
    columns[0] = jnp.concatenate([mean] * (HEAD_DIM // 8), axis=0).T
    columns[1] = jnp.concatenate([scale] * (HEAD_DIM // 8), axis=0).T

    def normalize(i, carry):
        at = pl.ds(i * 32, 32)
        x = acc[at, :]
        scaled = (x - columns[0, at, 0:1]) * columns[1, at, 0:1]
        normed[0, at, :] = (scaled * gain[...][None, :]).astype(jnp.bfloat16)
        return carry

    lax.fori_loop(0, rows // 32, normalize, 0, unroll=UNROLL)

    piece = rows // PIECES

    def norm_copy(slot, to, offset, i):
        at = pl.ds(i * piece, piece)
        return pltpu.make_async_remote_copy(
            src_ref=normed.at[slot, at], dst_ref=normed.at[to, at], send_sem=norm_send.at[to],
            recv_sem=norm_recv.at[to, i], device_id=(d ^ offset, z), device_id_type=MESH,
        )

    near, far = image_of(1, core), image_of(2, core)
    for p in (near, 1):
        for i in range(PIECES):
            norm_copy(0, p, p, i).start()


    def ready(c, i):
        @pl.when((lax.rem(c, 2) == 1) & (c < CHUNKS - 1))
        def _():
            p = image_of((c + 1) // 2, core)
            norm_copy(0, p, p, i).wait_recv()

            @pl.when(lax.rem(p, 2) == 0)
            def _():
                norm_copy(p, p + 1, 1, i).start()

    def sum_copy(t, c, i):
        part = sums.at[t, c, i * piece : (i + 1) * piece]
        return pltpu.make_async_remote_copy(
            src_ref=part, dst_ref=part, send_sem=sum_send.at[t],
            recv_sem=sum_recv.at[t, lax.rem(c, TURNS), i], device_id=(d, lax.rem(z + 2 * t - 1 + LINE, LINE)),
            device_id_type=MESH,
        )

    def give_copy(t, c, i):
        part = given.at[t, c, i * piece : (i + 1) * piece]
        return pltpu.make_async_remote_copy(
            src_ref=part, dst_ref=part, send_sem=give_send.at[t],
            recv_sem=give_recv.at[t, lax.rem(c, TURNS), i], device_id=(d, lax.rem(z + 1 - 2 * t + LINE, LINE)),
            device_id_type=MESH,
        )

    def part_copy(p):
        return pltpu.make_async_remote_copy(
            src_ref=sent.at[p - 1], dst_ref=got.at[p - 1], send_sem=part_send.at[p - 1],
            recv_sem=part_recv.at[p - 1], device_id=(d ^ p, z), device_id_type=MESH,
        )

    def term(c, t, at):
        return jnp.dot(
            normed[image_of((c + 1) // 2, core), at, :], wv[2 * t + lax.rem(c + 1, 2)], preferred_element_type=jnp.float32
        )

    def prepare(k):
        def one(t, carry):
            s = position(t)
            c = k - s

            @pl.when((s > 0) & (c >= 0) & (c < CHUNKS))
            def _():
                @pl.when(s == 1)
                def _():
                    for i in range(PIECES):
                        ready(c, i)

                terms[t] = term(c, t, slice(None))

            return carry

        lax.fori_loop(0, 2, one, 0)

    for item in loads[1:]:
        item.wait()

    def head_unit(values):
        mean = jnp.mean(values, axis=-1, keepdims=True)
        centered = values - mean
        spread = jnp.mean(centered * centered, axis=-1, keepdims=True)
        return centered * lax.rsqrt(spread + EPS)

    def finish(t, c):
        def column(i):
            value = terms[t, :, i * HEAD_DIM : (i + 1) * HEAD_DIM]
            value = value + sums[t, c, :, i * HEAD_DIM : (i + 1) * HEAD_DIM].astype(jnp.float32)
            return value.astype(jnp.bfloat16)

        query = head_unit(column(0).astype(jnp.float32)) * (1.0 / HEAD_DIM) ** 0.5
        keys = head_unit(column(1).astype(jnp.float32)).astype(jnp.bfloat16)
        scores = lax.dot_general(
            query.astype(jnp.bfloat16), keys, (((1,), (1,)), ((), ())), preferred_element_type=jnp.float32
        )
        weights = jnp.exp(scores)
        probs = (weights / jnp.sum(weights, axis=-1, keepdims=True)).astype(jnp.bfloat16)
        mixed = jnp.dot(probs, column(2), preferred_element_type=jnp.float32)
        given[t, c, :, :HEAD_DIM] = mixed.astype(jnp.bfloat16)
        for i in range(up_block // HEAD_DIM):
            u = column(3 + i).astype(jnp.float32)
            given[t, c, :, (1 + i) * HEAD_DIM : (2 + i) * HEAD_DIM] = jax.nn.gelu(u).astype(jnp.bfloat16)

    def sent_from(whole, sem):
        pltpu.make_async_remote_copy(
            src_ref=whole, dst_ref=whole, send_sem=sem, recv_sem=sem,
            device_id=(d, lax.rem(z + 1, LINE)), device_id_type=MESH,
        ).wait_send()

    inner = (z > 0) & (z < LINE - 1)

    def step(k, carry):
        def stream(n):
            far = jnp.where(z < LINE // 2, 1 - n, n)
            return jnp.where(inner, 1 - far, far)

        def move_sums(t, i):
            s = position(t)
            c = k - s

            @pl.when((c >= 0) & (c < CHUNKS))
            def _():
                at = pl.ds(i * piece, piece)

                @pl.when(s > 0)
                def _():
                    sum_copy(t, c, i).wait_recv()

                @pl.when(s == 0)
                def _():
                    ready(c, i)
                    sums[t, c, at, :] = term(c, t, at).astype(jnp.bfloat16)
                    sum_copy(t, c, i).start()

                @pl.when((s > 0) & (s < LINE - 1))
                def _():
                    value = terms[t, at, :] + sums[t, c, at, :].astype(jnp.float32)
                    sums[t, c, at, :] = value.astype(jnp.bfloat16)
                    sum_copy(t, c, i).start()

                if i == PIECES - 1:

                    @pl.when(s == LINE - 1)
                    def _():
                        finish(t, c)
                        for j in range(PIECES):
                            give_copy(t, c, j).start()

        def move_given(t, c):
            @pl.when((c >= 0) & (c < CHUNKS))
            def _():
                for i in range(PIECES):
                    give_copy(t, c, i).wait_recv()
                    give_copy(t, c, i).start()

        def serve(n, carry):
            t = stream(n)
            for i in range(PIECES):
                move_sums(t, i)

            @pl.when(n == 1)
            def _():
                prepare(k + 1)

            c = k - 2 * (LINE - 1) + 1

            @pl.when(inner & ((n == 1) | (k <= CHUNKS + 2)))
            def _():
                move_given(t, c)

            @pl.when(inner & (n == 0) & (k >= CHUNKS + 2))
            def _():
                move_given(t, c + 1)

            return carry

        lax.fori_loop(0, 2, serve, 0)

        @pl.when(k == 1)
        def _():
            sent_from(normed.at[0], norm_send.at[near])
            for i in range(PIECES):
                norm_copy(0, far, far, i).start()

        @pl.when(k == 3)
        def _():
            for i in range(PIECES):
                norm_copy(0, 6, 6, i).start()

        @pl.when(jnp.logical_not(inner) & (k >= 2 * (LINE - 1)))
        def _():
            for i in range(PIECES):
                give_copy(stream(0), k - 2 * (LINE - 1), i).wait_recv()

        c = k - 2 * (LINE - 1) + jnp.minimum(z, LINE - 1 - z)

        def tiles(work):
            def one(n, carry):
                work(pl.ds(n * 256, 256))
                return carry

            lax.fori_loop(0, out_cols // 256, one, 0)

        def own(t, c):
            def one(at):
                acc[:, at] = acc[:, at] + jnp.dot(
                    given[t, c], wo[2 * t + lax.rem(c + 1, 2), :, at], preferred_element_type=jnp.float32
                )

            tiles(one)

        @pl.when((c == 0) | (c == CHUNKS - 1))
        def _():
            own(stream(0), c)

            @pl.when((c == 0) | inner)
            def _():
                own(stream(1), c)

        @pl.when((c == CHUNKS - 3) & jnp.logical_not(inner))
        def _():
            own(stream(1), CHUNKS - 1)

        @pl.when((c >= 2) & (c < CHUNKS) & (lax.rem(c, 2) == 0))
        def _():
            p = image_of(c // 2, core)

            def other(at):
                value = jnp.zeros((rows, 256), jnp.float32)
                for t in range(2):
                    for h, chunk in enumerate((c - 1, c)):
                        value = value + jnp.dot(
                            given[t, chunk], wo[2 * t + h, :, at], preferred_element_type=jnp.float32
                        )
                sent[p - 1, :, at] = value.astype(jnp.bfloat16)

            tiles(other)
            part_copy(p).start()

            @pl.when((c >= 4) & (c < CHUNKS - 2))
            def _():
                collect(c // 2 - 1)

        return carry

    def arrival(pair):
        p = pick(pair, ORDER)
        return image_of(pair, jnp.where(lax.rem(p, 2) == 1, 1 - core, core))

    def collect(pair):
        p = arrival(pair)
        part_copy(p).wait_recv()

        def add(i, carry):
            at = pl.ds(i * 32, 32)
            acc[at, :] = acc[at, :] + got[p - 1, at, :].astype(jnp.float32)
            return carry

        lax.fori_loop(0, rows // 32, add, 0)

    lax.fori_loop(0, CHUNKS + 2 * (LINE - 1), step, 0)

    last = arrival(CHUNKS // 2 - 2)
    part_copy(last).wait_recv()
    part_copy(1).wait_recv()

    def write(i, carry):
        at = pl.ds(i * 32, 32)
        value = acc[at, :] + got[last - 1, at, :].astype(jnp.float32)
        out[at, :] = (value + got[0, at, :].astype(jnp.float32)).astype(jnp.bfloat16)
        return carry

    lax.fori_loop(0, rows // 32, write, 0)

    for r in range(1, LINE):
        stat_copy(r).wait_send()
    for p in (1, far, 6):
        sent_from(normed.at[0], norm_send.at[p])
    for p in (2, 4, 6):
        sent_from(normed.at[p], norm_send.at[p + 1])

    for t in range(2):

        @pl.when(position(t) < LINE - 1)
        def _():
            sent_from(sums.at[t], sum_send.at[t])

        @pl.when(position(t) > 0)
        def _():
            sent_from(given.at[t], give_send.at[t])

    for p in range(1, IMAGES):
        part_copy(p).wait_send()


def on_line(tokens, norm_gain, w_qkv, w_up, w_attn_out, w_down):
    rows, feat = tokens.shape
    units = w_up.shape[1]
    up_block = units // BLOCKS
    out_cols = w_down.shape[1]
    cols = 3 * HEAD_DIM + up_block
    hidden = HEAD_DIM + up_block
    w_heads = w_qkv.transpose(1, 0, 2)
    anywhere = pl.BlockSpec(memory_space=pl.ANY)
    inside = pl.BlockSpec(memory_space=pltpu.VMEM)
    dma = pltpu.SemaphoreType.DMA
    return pl.pallas_call(
        line_kernel,
        out_shape=pltpu.VMEM((rows, out_cols), jnp.bfloat16),
        in_specs=[anywhere, inside] + [anywhere] * 4,
        out_specs=inside,
        scratch_shapes=[
            pltpu.VMEM((rows, feat), jnp.bfloat16),
            pltpu.VMEM((BLOCKS, feat, cols), jnp.bfloat16),
            pltpu.VMEM((BLOCKS, hidden, out_cols), jnp.bfloat16),
            pltpu.VMEM((IMAGES, rows, feat), jnp.bfloat16),
            pltpu.VMEM((2, CHUNKS, rows, cols), jnp.bfloat16),
            pltpu.VMEM((2, CHUNKS, rows, hidden), jnp.bfloat16),
            pltpu.VMEM((IMAGES - 1, rows, out_cols), jnp.bfloat16),
            pltpu.VMEM((IMAGES - 1, rows, out_cols), jnp.bfloat16),
            pltpu.VMEM((2, rows, cols), jnp.float32),
            pltpu.VMEM((rows, out_cols), jnp.float32),
            pltpu.VMEM((2, rows, HEAD_DIM), jnp.float32),
            pltpu.VMEM((16, rows), jnp.float32),
            pltpu.VMEM((LINE - 1, 16, rows), jnp.float32),
            dma((1 + 6 * BLOCKS,)),
            dma((LINE - 1,)),
            dma((LINE - 1,)),
            dma((IMAGES,)),
            dma((IMAGES, PIECES)),
            dma((2,)),
            dma((2, TURNS, PIECES)),
            dma((2,)),
            dma((2, TURNS, PIECES)),
            dma((IMAGES - 1,)),
            dma((IMAGES - 1,)),
        ],
        compiler_params=pltpu.CompilerParams(
            collective_id=0, has_side_effects=True, vmem_limit_bytes=66_000_000
        ),
    )(tokens, norm_gain, w_heads, w_up, w_attn_out, w_down)


def solution(mesh):
    placed = (
        P("dp", "mp"),
        P("mp"),
        P("mp", None, "dp"),
        P("mp", "dp"),
        P("dp", "mp"),
        P("dp", "mp"),
    )
    return jax.shard_map(
        local, mesh=mesh, in_specs=placed, out_specs=P("dp", "mp"), check_vma=False
    )
```
